32 devices in a mesh: band: 8 (over y, x, core), pw: 4 (over z).
Axes of the slice: x: 2, y: 2, z: 4, core: 2. Of those that a mesh axis runs over, the one named last changes fastest.
Arguments:
- pair_density: bfloat16 [40, 128, 9216], P('band', None, 'pw'), may hold values from -6 to 6
- eigvecs: bfloat16 [2944, 9216], P('band', 'pw'), may hold values from -0.0625 to 0.0625
- screening: bfloat16 [2944, 2944], P('pw'), may hold values from -0.00048828125 to 0.00048828125
- occupation: float32 [16], replicated, may hold values from 0 to 1
- window_start: int32 [40], P('band'), may hold values from 0 to 511, as said below
- window_len: int32 [40], P('band'), may hold values from 1 to 128, as said below
- slot_band: int32 [40], P('band'), may hold values from -1 to 15, as said below
Outputs:
- sigma: float32 [512, 512], P(('band', 'pw'))
The draws below stay inside these ranges and needn't reach their ends.
Inputs may be any that keep to these rules, and one draw needn't show every extreme that they name: window_start + window_len <= 512 for every slot. `window_len`: some slot has a window of 128 bands. On each index of band the live slots (slot_band >= 0) come first among its 5 slots; each index holds 3 to 5 live slots, and the counts of index i and index i + 8 / 2 add up to 8.
All inputs are finite; a program needn't handle non-finite values.
Results may differ from the reference program's by a relative error of at most 0.0049.
Values may be sent and summed in bfloat16 or wider, within the bound.
A program may use at most 128 MiB of HBM per device.

```python
import jax
import jax.numpy as jnp
from jax import lax

NB_SIGMA = 512
BLOCK = 128
G = 9216
S = 2944
CAP = 5
SLOTS = 40
NSUM = 16


def window_parts(key):
    lengths = jax.random.randint(jax.random.fold_in(key, 11), (SLOTS,), 1, BLOCK + 1)
    lengths = lengths.at[0].set(BLOCK)
    lengths = lengths.at[1].set(1)
    spaces = NB_SIGMA - lengths + 1
    raw_bits = jax.random.randint(jax.random.fold_in(key, 12), (SLOTS,), 0, 1 << 30)
    starts = raw_bits % spaces
    starts = starts.at[0].set(0)
    starts = starts.at[1].set(NB_SIGMA - 1)
    return (starts.astype(jnp.int32), lengths.astype(jnp.int32))


def draw_window_start(key, part):
    starts, lengths = window_parts(key)
    return starts


def draw_window_len(key, part):
    starts, lengths = window_parts(key)
    return lengths


def draw_slot_band(key, part):
    groups = SLOTS // CAP
    halves = groups // 2
    lower = jax.random.randint(jax.random.fold_in(key, 21), (halves,), CAP - 2, CAP + 1)
    counts = jnp.concatenate([lower, 2 * CAP - 2 - lower])
    position = jnp.arange(SLOTS, dtype=jnp.int32) % CAP
    device = jnp.arange(SLOTS, dtype=jnp.int32) // CAP
    band_ids = jax.random.randint(jax.random.fold_in(key, 22), (SLOTS,), 0, NSUM)
    return jnp.where(position < counts[device], band_ids, -1).astype(jnp.int32)


def steps_of(own_key, extent, pieces, least, top_value):
    def one(axis_at, parts):
        heights = jax.random.uniform(jax.random.fold_in(jax.random.fold_in(own_key, 6), axis_at), (parts,), jnp.float32, least / len(pieces), top_value / len(pieces))
        return jnp.repeat(jnp.exp(heights), extent[axis_at] // parts).reshape((-1,) + (1,) * (len(extent) - axis_at - 1))

    level = one(*pieces[0])
    for cut in pieces[1:]:
        level = level * one(*cut)
    return level


def noise(own_key, shape, width, bound, pieces=(), kind=jnp.bfloat16):
    result = jax.random.normal(own_key, shape, jnp.float32) * width
    if len(pieces) > 0:
        result = steps_of(own_key, shape, pieces, -0.22, 0.18) * result
    return jnp.clip(result, min=-bound, max=bound).astype(kind)


def setup_inputs(seed: int = 0) -> dict:
    streams_of = jax.random.split(jax.random.key(seed), 8)
    return {
        "pair_density": noise(streams_of[0], (SLOTS, BLOCK, G), 1.0, 6.0, ((0, 8), (2, 4))),
        "eigvecs": noise(streams_of[1], (S, G), G ** -0.5, 0.0625, ((0, 8), (1, 4))),
        "screening": noise(streams_of[2], (S, S), (16 * S * S) ** -0.5, 0.00048828125, ((0, 4),)),
        "occupation": jnp.clip(jax.random.uniform(streams_of[3], (NSUM,), jnp.float32, 0.0, 1.0), 0.0, 1.0),
        "window_start": draw_window_start(jax.random.fold_in(streams_of[7], 71), 0),
        "window_len": draw_window_len(jax.random.fold_in(streams_of[7], 71), 0),
        "slot_band": draw_slot_band(jax.random.fold_in(streams_of[7], 71), 0),
    }


def reference(pair_density, eigvecs, screening, occupation, window_start, window_len, slot_band):
    row_ids = jnp.arange(BLOCK, dtype=jnp.int32)
    band_list = jnp.arange(NSUM, dtype=jnp.int32)

    def add_slot(totals, item):
        density, offset, length, band_id = item
        raw_proj = jnp.dot(density, eigvecs.T, preferred_element_type=jnp.float32)
        keep_rows = ((row_ids < length) & (band_id >= 0)).astype(jnp.float32)
        projected = (raw_proj * keep_rows[:, None]).astype(jnp.bfloat16)
        screened = jnp.dot(projected, screening.T, preferred_element_type=jnp.float32).astype(jnp.bfloat16)
        block_sigma = jnp.dot(screened, projected.T, preferred_element_type=jnp.float32)
        weight = 0.5 - jnp.sum(jnp.where(band_list == band_id, occupation, jnp.zeros_like(occupation)))
        first = offset.astype(jnp.int32)
        previous = lax.dynamic_slice(totals, (first, first), (BLOCK, BLOCK))
        totals = lax.dynamic_update_slice(totals, previous + weight * block_sigma, (first, first))
        return totals, None

    start_sum = jnp.zeros((NB_SIGMA + BLOCK, NB_SIGMA + BLOCK), jnp.float32)
    totals, unused = lax.scan(add_slot, start_sum, (pair_density, window_start, window_len, slot_band))
    return totals[:NB_SIGMA, :NB_SIGMA]
```

```python
import functools

import jax
import jax.numpy as jnp
from jax import lax
from jax.experimental import pallas as pl
from jax.experimental.pallas import tpu as pltpu
from jax.sharding import PartitionSpec as P

NB_SIGMA = 512


def ring_per_device(pair_density, eigvecs, screening, occupation, window_start, window_len, slot_band):
    capacity, block, plane_rows = pair_density.shape
    density, starts, lengths, band_ids = (pair_density, window_start, window_len, slot_band)
    slots = density.shape[0]
    flat = density.reshape(slots * block, plane_rows)
    partial_proj = lax.dot_general(
        flat,
        lax.all_gather(eigvecs, "band", axis=0, tiled=True),
        (((1,), (1,)), ((), ())),
        preferred_element_type=jnp.float32,
    )
    row_ids = jnp.arange(block, dtype=jnp.int32)
    keep_rows = ((row_ids[None, :] < lengths[:, None]) & (band_ids[:, None] >= 0)).astype(
        jnp.float32
    )
    masked = partial_proj * keep_rows.reshape(slots * block, 1)
    projected = lax.psum(masked, "pw").astype(jnp.bfloat16)
    width = screening.shape[0]
    own_cols = lax.dynamic_slice_in_dim(projected, lax.axis_index("pw") * width, width, 1)
    screened = lax.dot_general(
        projected, screening, (((1,), (1,)), ((), ())), preferred_element_type=jnp.float32
    ).astype(jnp.bfloat16)
    block_sigma = lax.dot_general(
        screened.reshape(slots, block, width),
        own_cols.reshape(slots, block, width),
        (((2,), (2,)), ((0,), (0,))),
        preferred_element_type=jnp.float32,
    )
    band_list = jnp.arange(occupation.shape[0], dtype=jnp.int32)
    weights = 0.5 - jnp.sum(
        jnp.where(band_list[None, :] == band_ids[:, None], occupation[None, :], 0.0), axis=1
    )
    totals = jnp.zeros((NB_SIGMA + block, NB_SIGMA + block), jnp.float32)
    for index in range(slots):
        first = starts[index]
        previous = lax.dynamic_slice(totals, (first, first), (block, block))
        totals = lax.dynamic_update_slice(
            totals, previous + weights[index] * block_sigma[index], (first, first)
        )
    sigma_part = totals[:NB_SIGMA, :NB_SIGMA]
    by_band = lax.psum_scatter(sigma_part, "band", scatter_dimension=0, tiled=True)
    return lax.psum_scatter(by_band, "pw", scatter_dimension=0, tiled=True)


def flip(index, relation):
    total = 0
    for place in (4, 2, 1):
        bit = lax.rem(index // place, 2)
        other = lax.rem(relation // place, 2)
        total = total + place * (bit + other - 2 * bit * other)
    return total


def split(value):
    top = value.astype(jnp.bfloat16)
    return top, (value - top.astype(jnp.float32)).astype(jnp.bfloat16)


N_QUARTER = 4
EARLY, PATCH, FULL = 2 * N_QUARTER, 2, 6 * N_QUARTER
TICKS = EARLY + PATCH + FULL
LAG_SUM, LAG_TOTAL, LAG_SCREEN = 2, 5, 8


def piece_of(order):
    pair, core = lax.div(order, 2), lax.rem(order, 2)
    late = lax.div(pair, 8)
    side = lax.rem(pair + 1, 2) + lax.div(pair, 7) - 1 + lax.div(pair + 7, 8)
    near = lax.rem(lax.div(pair + 1, 2), 4)
    rest = pair - 8 * late
    corner = lax.rem(rest + 1, 3) + 2 * lax.div(rest, 3)
    relation = (1 - late) * (2 + 2 * side) + late * 6 + core
    return relation, (1 - late) * near + late * corner


def fused_kernel(
    density_ref, eig_ref, screen_ref, start_ref, len_ref, slot_ref, occ_ref, out_ref,
    density, extra, extra_out, extra_meta, meta, keep, eig, stage, screen, part, sent, from_edge, from_mid,
    proj, acc, place, high, low, sig_out, sig_own, sig_in, xy_in, band_sum, fin_in,
    load_sem, swap_send, swap_recv, eig_send, eig_recv, z_send, z_recv, sig_send, sig_recv, xy_send, xy_recv,
    fin_send, fin_recv,
):
    mesh_id = pl.DeviceIdType.MESH
    band, z = lax.axis_index("band"), lax.axis_index("pw")
    n_rel, padded, _ = eig.shape
    depth = eig_ref.shape[0]
    piece = padded // N_QUARTER
    short = depth - (N_QUARTER - 1) * piece
    block = extra.shape[0]
    cols = density.shape[0]
    slots = cols // block
    most = cols - block
    n_z = fin_in.shape[0] + 1
    mate, across = z + 1 - 2 * lax.rem(z, 2), n_z - 1 - z
    inner = (z == 1) | (z == 2)
    edge = (z == 0) | (z == n_z - 1)
    whole_rows = pl.ds(0, depth)

    loads = [
        pltpu.make_async_copy(eig_ref, eig.at[0, whole_rows], load_sem.at[0]),
        pltpu.make_async_copy(density_ref.at[pl.ds(0, cols)], density, load_sem.at[1]),
        pltpu.make_async_copy(screen_ref, stage, load_sem.at[2]),
    ]
    for load in loads:
        load.start()

    def fields(slot):
        live = slot_ref[slot] >= 0
        kept = jnp.where(live, len_ref[slot], 0).astype(jnp.float32)
        weight = jnp.where(live, 0.5 - occ_ref[jnp.maximum(slot_ref[slot], 0)], 0.5)
        first = start_ref[slot].astype(jnp.float32)
        row = lax.broadcasted_iota(jnp.int32, (8, block), 0)
        return jnp.where(row == 0, kept, jnp.where(row == 1, weight, first))

    extra_out[...] = fields(slots)
    for slot in range(slots):
        meta[slot] = fields(slot)

    barrier = pltpu.get_barrier_semaphore()
    for rel in range(1, n_rel):
        pl.semaphore_signal(barrier, inc=1, device_id=(flip(band, rel), z), device_id_type=mesh_id)
    for k in range(1, n_z):
        pl.semaphore_signal(
            barrier, inc=1, device_id=(band, lax.rem(z + k, n_z)), device_id_type=mesh_id
        )
    tail = pl.ds(depth, padded - depth)
    for rel in range(n_rel):
        eig[rel, tail] = jnp.zeros((padded - depth, eig.shape[2]), eig.dtype)
        for buffer in (from_edge, from_mid, proj):
            buffer[rel, tail] = jnp.zeros((padded - depth, cols), buffer.dtype)
    acc[...] = jnp.zeros_like(acc)
    lanes = lax.broadcasted_iota(jnp.int32, (8, block), 1).astype(jnp.float32)
    for slot in range(slots):
        keep[:, slot * block : (slot + 1) * block] = jnp.where(lanes < meta[slot, 0:1], 1.0, 0.0)
    pl.semaphore_wait(barrier, n_rel - 1 + n_z - 1)

    def remote(source, target, send, recv, device):
        return pltpu.make_async_remote_copy(
            src_ref=source, dst_ref=target, send_sem=send, recv_sem=recv,
            device_id=device, device_id_type=mesh_id,
        )

    def rows_at(quarter, rows):
        if isinstance(quarter, int):
            return pl.ds(quarter * piece, rows)
        return pl.ds(pl.multiple_of(quarter * piece, 16), rows)

    def each(quarter, act):
        if isinstance(quarter, int):
            act(rows_at(quarter, piece if quarter < N_QUARTER - 1 else short))
            return

        @pl.when(quarter < N_QUARTER - 1)
        def _():
            act(rows_at(quarter, piece))

        @pl.when(quarter == N_QUARTER - 1)
        def _():
            act(rows_at(quarter, short))

    def own_copy(rel, quarter, rows):
        return remote(
            eig_ref.at[rows], eig.at[rel, rows], eig_send.at[rel, quarter],
            eig_recv.at[rel, quarter], (flip(band, rel), z),
        )

    def forward_copy(rel, quarter, rows):
        return remote(
            eig.at[rel, rows], eig.at[rel + 1, rows], eig_send.at[rel + 1, quarter],
            eig_recv.at[rel + 1, quarter], (flip(band, 1), z),
        )

    def corner_copy(via, quarter, rows):
        return remote(
            eig.at[via, rows], eig.at[6, rows], eig_send.at[6, quarter],
            eig_recv.at[6, quarter], (flip(band, 6 - via), z),
        )

    def landed(rel, quarter, rows):
        return remote(
            eig.at[rel, rows], eig.at[rel, rows], eig_send.at[rel, quarter],
            eig_recv.at[rel, quarter], (flip(band, 1), z),
        )

    def z_copy(kind, rel, quarter, rows, columns):
        source, target = ((sent, from_edge), (sent, from_mid), (proj, proj))[kind]
        return remote(
            source.at[rel, rows, columns], target.at[rel, rows, columns],
            z_send.at[kind, rel, quarter], z_recv.at[kind, rel, quarter],
            (band, across if kind == 1 else mate),
        )

    swaps = [
        remote(source, target, swap_send.at[index], swap_recv.at[index], (flip(band, 4), z))
        for index, (source, target) in enumerate(
            [(density_ref.at[pl.ds(cols, block)], extra), (extra_out, extra_meta)]
        )
    ]
    for swap in swaps:
        swap.start()
    for index in range(N_QUARTER):
        for rel, quarter in ((1, index), (2, index), (4, (index + 1) % N_QUARTER)):
            each(quarter, lambda rows: own_copy(rel, quarter, rows).start())

    first_cols, last_cols, all_cols = pl.ds(0, most), pl.ds(most, block), pl.ds(0, cols)

    def items(index, whole, act):
        @pl.when((index >= 0) & (index < EARLY))
        def _():
            rel, quarter = lax.rem(index, 2), lax.div(index, 2)
            act(rel, quarter, rows_at(quarter, piece), first_cols, lambda do: each(quarter, do))

        @pl.when((index >= EARLY) & (index < EARLY + PATCH))
        def _():
            act(
                index - EARLY, N_QUARTER, pl.ds(0, padded), last_cols, lambda do: do(whole_rows)
            )

        @pl.when((index >= EARLY + PATCH) & (index < TICKS))
        def _():
            rel, quarter = piece_of(index - EARLY - PATCH)
            act(rel, quarter, rows_at(quarter, piece), all_cols, lambda do: each(quarter, do))

    def arrive(index):
        @pl.when((index < EARLY) & (lax.rem(index, 2) == 1))
        def _():
            quarter = lax.div(index, 2)
            each(quarter, lambda rows: landed(1, quarter, rows).wait_recv())

        @pl.when(index == EARLY)
        def _():
            for swap in swaps:
                swap.wait_recv()
            taken = meta[slots - 1, 0:1, 0:1] > 0.0
            meta[slots - 1] = jnp.where(taken, meta[slots - 1], extra_meta[...])
            density[most:] = jnp.where(taken, density[most:], extra[...])
            keep[:, most:] = jnp.where(lanes < meta[slots - 1, 0:1], 1.0, 0.0)

        @pl.when((index >= EARLY + PATCH) & (index < TICKS))
        def _():
            rel, quarter = piece_of(index - EARLY - PATCH)
            each(quarter, lambda rows: landed(rel, quarter, rows).wait_recv())

            @pl.when(lax.rem(rel, 2) == 0)
            def _():
                each(quarter, lambda rows: forward_copy(rel, quarter, rows).start())

            @pl.when((rel == 2) & (quarter == 0))
            def _():
                corner_copy(2, 0, pl.ds(0, piece)).start()

            @pl.when((rel == 4) & (quarter > 0))
            def _():
                each(quarter, lambda rows: corner_copy(4, quarter, rows).start())

    def project(rel, quarter, rows, columns, sizes):
        result = lax.dot_general(
            eig[rel, rows], density[columns], (((1,), (1,)), ((), ())),
            preferred_element_type=jnp.float32,
        )
        part[rel, rows, columns] = result
        sent[rel, rows, columns] = result.astype(jnp.bfloat16)

        @pl.when(edge)
        def _():
            sizes(lambda dma_rows: z_copy(0, rel, quarter, dma_rows, columns).start())

    def add_edge(rel, quarter, rows, columns, sizes):
        sizes(lambda dma_rows: z_copy(0, rel, quarter, dma_rows, columns).wait_recv())
        total = part[rel, rows, columns] + from_edge[rel, rows, columns].astype(jnp.float32)
        part[rel, rows, columns] = total
        sent[rel, rows, columns] = total.astype(jnp.bfloat16)
        sizes(lambda dma_rows: z_copy(1, rel, quarter, dma_rows, columns).start())

    def add_mid(rel, quarter, rows, columns, sizes):
        sizes(lambda dma_rows: z_copy(1, rel, quarter, dma_rows, columns).wait_recv())
        total = part[rel, rows, columns] + from_mid[rel, rows, columns].astype(jnp.float32)
        proj[rel, rows, columns] = (total * keep[0:1, columns]).astype(jnp.bfloat16)
        sizes(lambda dma_rows: z_copy(2, rel, quarter, dma_rows, columns).start())

    def apply_screen(rel, quarter):
        acc[...] += lax.dot_general(
            proj[rel, rows_at(quarter, piece)], screen[flip(band, rel), quarter],
            (((0,), (1,)), ((), ())), preferred_element_type=jnp.float32,
        )

    def screen_early(index):
        rel, quarter = lax.rem(index, 2), lax.div(index, 2)

        @pl.when(edge)
        def _():
            each(quarter, lambda rows: z_copy(2, rel, quarter, rows, first_cols).wait_recv())

            @pl.when(quarter == 0)
            def _():
                z_copy(2, rel, N_QUARTER, whole_rows, last_cols).wait_recv()

        apply_screen(rel, quarter)

    def screen_full(index):
        rel, quarter = piece_of(index)

        @pl.when(edge)
        def _():
            each(quarter, lambda rows: z_copy(2, rel, quarter, rows, all_cols).wait_recv())

        apply_screen(rel, quarter)

    width = screen_ref.shape[0] // 2

    def arrange_screen(at):
        for quarter in range(N_QUARTER):
            rows = piece if quarter < N_QUARTER - 1 else short
            left = at * depth + quarter * piece
            for half in range(2):
                picked = stage[half * width : (half + 1) * width, left : left + rows]
                if rows < piece:
                    picked = jnp.concatenate(
                        [picked, jnp.zeros((width, piece - rows), picked.dtype)], axis=1
                    )
                screen[at, quarter, half * padded : half * padded + width] = picked
                screen[at, quarter, half * padded + width : (half + 1) * padded] = jnp.zeros(
                    (padded - width, piece), picked.dtype
                )

    strip = place.shape[1]

    def build_place():
        for slot in range(slots):
            here = slice(slot * block, (slot + 1) * block)
            window = lax.broadcasted_iota(jnp.int32, (strip, block), 1).astype(jnp.float32)
            window = window + meta[slot, 2:3]
            bands = lax.broadcasted_iota(jnp.int32, (strip, block), 0).astype(jnp.float32)
            for index in range(n_rel):
                same = bands + float(index * strip) == window
                place[index, :, here] = jnp.where(same, 1.0, 0.0).astype(jnp.bfloat16)

    def step(t, carry):
        arrive(t)
        items(t, True, project)

        @pl.when(inner)
        def _():
            items(t - LAG_SUM, True, add_edge)
            items(t - LAG_TOTAL, True, add_mid)

        for at in range(n_rel):
            @pl.when(t == 4 + at)
            def _():
                if at == 0:
                    loads[2].wait()
                arrange_screen(at)

        @pl.when(t == EARLY + 4)
        def _():
            build_place()

        early = t - EARLY - PATCH - LAG_SCREEN

        @pl.when((early >= 0) & (early < EARLY))
        def _():
            screen_early(early)

        full = t - EARLY - PATCH - LAG_SCREEN

        @pl.when((full >= 0) & (full < FULL))
        def _():
            screen_full(full)

        return carry

    loads[0].wait()
    loads[1].wait()
    lax.fori_loop(0, TICKS + LAG_SCREEN, step, 0)

    pair = [proj.at[flip(band, 2 * z + half)] for half in range(2)]
    for slot in range(slots):
        here = slice(slot * block, (slot + 1) * block)
        total = 0.0
        for value in split(acc[here]):
            for half in range(2):
                total = total + jnp.dot(
                    value[:, half * padded : (half + 1) * padded], pair[half][:, here],
                    preferred_element_type=jnp.float32,
                )
        spread = 0.0
        for value in split(total * meta[slot, 1:2]):
            spread = spread + lax.dot_general(
                value, place[:, :, here].reshape(n_rel * strip, block), (((1,), (1,)), ((), ())),
                preferred_element_type=jnp.float32,
            )
        high[here], low[here] = split(spread)

    core = lax.rem(band, 2)
    chip = lax.div(band, 2)

    def strips(parity):
        rows = jnp.concatenate([place[2 * index + parity] for index in range(n_rel // 2)], axis=0)
        return sum(
            jnp.dot(rows, value[...], preferred_element_type=jnp.float32) for value in (high, low)
        ).reshape(sig_out.shape)

    sig_out[...] = strips(1 - core)
    core_copy = remote(sig_out, sig_in, sig_send, sig_recv, (flip(band, 1), z))
    core_copy.start()
    sig_own[...] = strips(core)

    def chip_copy(rel):
        target = flip(band, 2 * rel)
        return remote(
            sig_own.at[lax.div(target, 2)], xy_in.at[rel - 1], xy_send.at[rel - 1],
            xy_recv.at[rel - 1], (target, z),
        )

    def final_copy(k):
        target = lax.rem(z + k, n_z)
        return remote(
            band_sum.at[target], fin_in.at[k - 1], fin_send.at[k - 1], fin_recv.at[k - 1],
            (band, target),
        )

    core_copy.wait_recv()
    sig_own[...] += sig_in[...]
    for rel in (3, 1, 2):
        chip_copy(rel).start()

    for swap in swaps:
        swap.wait_send()

    def drain(rel, carry):
        for quarter in range(N_QUARTER):
            rows = rows_at(quarter, piece if quarter < N_QUARTER - 1 else short)

            @pl.when(rel > 0)
            def _():
                landed(rel, quarter, rows).wait_send()

            def drain_z(columns):
                @pl.when(edge)
                def _():
                    z_copy(0, rel, quarter, rows, columns).wait_send()

                @pl.when(inner)
                def _():
                    z_copy(1, rel, quarter, rows, columns).wait_send()
                    z_copy(2, rel, quarter, rows, columns).wait_send()

            @pl.when(rel < 2)
            def _():
                drain_z(first_cols)

            @pl.when(rel >= 2)
            def _():
                drain_z(all_cols)

        @pl.when((rel < 2) & edge)
        def _():
            z_copy(0, rel, N_QUARTER, whole_rows, last_cols).wait_send()

        @pl.when((rel < 2) & inner)
        def _():
            z_copy(1, rel, N_QUARTER, whole_rows, last_cols).wait_send()
            z_copy(2, rel, N_QUARTER, whole_rows, last_cols).wait_send()

        return carry

    lax.fori_loop(0, n_rel, drain, 0)
    core_copy.wait_send()

    total = sig_own[chip]
    for rel in range(1, 4):
        chip_copy(rel).wait_recv()
        total = total + xy_in[rel - 1]
    band_sum[...] = total.reshape(band_sum.shape)
    for k in (2, 1, 3):
        final_copy(k).start()
    total = band_sum[z]
    for k in range(1, n_z):
        final_copy(k).wait_recv()
        total = total + fin_in[k - 1]
    out_ref[...] = total
    for rel in range(1, 4):
        chip_copy(rel).wait_send()
    for k in range(1, n_z):
        final_copy(k).wait_send()


def per_device(
    n_z, n_rel, pair_density, eigvecs, screening, occupation, window_start, window_len, slot_band
):
    capacity, block, plane_rows = pair_density.shape
    depth, width = eigvecs.shape[0], screening.shape[0]
    slots = capacity - 1
    cols = slots * block
    piece = -(-depth // (16 * N_QUARTER)) * 16
    padded = N_QUARTER * piece
    dma = pltpu.SemaphoreType.DMA
    vmem = pl.BlockSpec(memory_space=pltpu.VMEM)
    smem = pl.BlockSpec(memory_space=pltpu.SMEM)
    hbm = pl.BlockSpec(memory_space=pl.ANY)
    strip = NB_SIGMA // n_rel
    fine = strip // n_z
    f32, bf16 = jnp.float32, jnp.bfloat16
    return pl.pallas_call(
        fused_kernel,
        out_shape=jax.ShapeDtypeStruct((fine, NB_SIGMA), f32),
        in_specs=[hbm, hbm, hbm, smem, smem, smem, smem],
        out_specs=vmem,
        scratch_shapes=[
            pltpu.VMEM((cols, plane_rows), bf16),
            pltpu.VMEM((block, plane_rows), bf16),
            pltpu.VMEM((8, block), f32),
            pltpu.VMEM((8, block), f32),
            pltpu.VMEM((slots, 8, block), f32),
            pltpu.VMEM((8, cols), f32),
            pltpu.VMEM((n_rel, padded, plane_rows), bf16),
            pltpu.VMEM((width, screening.shape[1]), bf16),
            pltpu.VMEM((n_rel, N_QUARTER, 2 * padded, piece), bf16),
            pltpu.VMEM((n_rel, padded, cols), f32),
            pltpu.VMEM((n_rel, padded, cols), bf16),
            pltpu.VMEM((n_rel, padded, cols), bf16),
            pltpu.VMEM((n_rel, padded, cols), bf16),
            pltpu.VMEM((n_rel, padded, cols), bf16),
            pltpu.VMEM((cols, 2 * padded), f32),
            pltpu.VMEM((n_rel, strip, cols), bf16),
            pltpu.VMEM((cols, NB_SIGMA), bf16),
            pltpu.VMEM((cols, NB_SIGMA), bf16),
            pltpu.VMEM((n_rel // 2, strip, NB_SIGMA), f32),
            pltpu.VMEM((n_rel // 2, strip, NB_SIGMA), f32),
            pltpu.VMEM((n_rel // 2, strip, NB_SIGMA), f32),
            pltpu.VMEM((n_rel // 2 - 1, strip, NB_SIGMA), f32),
            pltpu.VMEM((n_z, fine, NB_SIGMA), f32),
            pltpu.VMEM((n_z - 1, fine, NB_SIGMA), f32),
            dma((3,)),
            dma((2,)),
            dma((2,)),
            dma((n_rel, N_QUARTER)),
            dma((n_rel, N_QUARTER)),
            dma((3, n_rel, N_QUARTER + 1)),
            dma((3, n_rel, N_QUARTER + 1)),
            dma,
            dma,
            dma((n_rel // 2 - 1,)),
            dma((n_rel // 2 - 1,)),
            dma((n_z - 1,)),
            dma((n_z - 1,)),
        ],
        compiler_params=pltpu.CompilerParams(
            collective_id=0, has_side_effects=True, vmem_limit_bytes=60 * 2**20
        ),
    )(
        pair_density.reshape(capacity * block, plane_rows),
        eigvecs,
        screening,
        window_start,
        window_len,
        slot_band,
        occupation,
    )


def solution(mesh):
    n_band, n_z = mesh.shape["band"], mesh.shape["pw"]
    body = ring_per_device
    if n_band == 8 and n_z == 4:
        body = functools.partial(per_device, n_z, n_band)
    return jax.shard_map(
        body,
        mesh=mesh,
        in_specs=(
            P("band", None, "pw"),
            P("band", "pw"),
            P("pw", None),
            P(),
            P("band"),
            P("band"),
            P("band"),
        ),
        out_specs=P(("band", "pw"), None),
        check_vma=False,
    )
```

```python
import functools

import jax
import jax.numpy as jnp
from jax import lax
from jax.experimental import pallas as pl
from jax.experimental.pallas import tpu as pltpu
from jax.sharding import PartitionSpec as P

NB_SIGMA = 512


def ring_per_device(pair_density, eigvecs, screening, occupation, window_start, window_len, slot_band):
    capacity, block, plane_rows = pair_density.shape
    density, starts, lengths, band_ids = (pair_density, window_start, window_len, slot_band)
    slots = density.shape[0]
    flat = density.reshape(slots * block, plane_rows)
    partial_proj = lax.dot_general(
        flat,
        lax.all_gather(eigvecs, "band", axis=0, tiled=True),
        (((1,), (1,)), ((), ())),
        preferred_element_type=jnp.float32,
    )
    row_ids = jnp.arange(block, dtype=jnp.int32)
    keep_rows = ((row_ids[None, :] < lengths[:, None]) & (band_ids[:, None] >= 0)).astype(
        jnp.float32
    )
    masked = partial_proj * keep_rows.reshape(slots * block, 1)
    projected = lax.psum(masked, "pw").astype(jnp.bfloat16)
    width = screening.shape[0]
    own_cols = lax.dynamic_slice_in_dim(projected, lax.axis_index("pw") * width, width, 1)
    screened = lax.dot_general(
        projected, screening, (((1,), (1,)), ((), ())), preferred_element_type=jnp.float32
    ).astype(jnp.bfloat16)
    block_sigma = lax.dot_general(
        screened.reshape(slots, block, width),
        own_cols.reshape(slots, block, width),
        (((2,), (2,)), ((0,), (0,))),
        preferred_element_type=jnp.float32,
    )
    band_list = jnp.arange(occupation.shape[0], dtype=jnp.int32)
    weights = 0.5 - jnp.sum(
        jnp.where(band_list[None, :] == band_ids[:, None], occupation[None, :], 0.0), axis=1
    )
    totals = jnp.zeros((NB_SIGMA + block, NB_SIGMA + block), jnp.float32)
    for index in range(slots):
        first = starts[index]
        previous = lax.dynamic_slice(totals, (first, first), (block, block))
        totals = lax.dynamic_update_slice(
            totals, previous + weights[index] * block_sigma[index], (first, first)
        )
    sigma_part = totals[:NB_SIGMA, :NB_SIGMA]
    by_band = lax.psum_scatter(sigma_part, "band", scatter_dimension=0, tiled=True)
    return lax.psum_scatter(by_band, "pw", scatter_dimension=0, tiled=True)


def flip(index, relation):
    total = 0
    for place in (4, 2, 1):
        bit = lax.rem(index // place, 2)
        other = lax.rem(relation // place, 2)
        total = total + place * (bit + other - 2 * bit * other)
    return total


def split(value):
    top = value.astype(jnp.bfloat16)
    return top, (value - top.astype(jnp.float32)).astype(jnp.bfloat16)


N_QUARTER = 4
EARLY, PATCH, FULL = 2 * N_QUARTER, 2, 6 * N_QUARTER
TICKS = EARLY + PATCH + FULL
LAG_SUM, LAG_TOTAL, LAG_SCREEN = 2, 4, 6
DONE = (8, 9, 20, 21, 24, 25, 32, 33)


def quarter_sizes(depth):
    units = depth // 16
    middle = -(-units // N_QUARTER)
    return 16 * (middle + 1), 16 * middle, 16 * middle, 16 * (units - 3 * middle - 1)


def piece_of(order):
    pair, core = lax.div(order, 2), lax.rem(order, 2)
    late = lax.div(pair, 8)
    side = lax.rem(pair + 1, 2) + lax.div(pair, 7) - 1 + lax.div(pair + 7, 8)
    near = lax.rem(lax.div(pair + 1, 2), 4)
    rest = pair - 8 * late
    corner = lax.rem(rest + 1, 3) + 2 * lax.div(rest, 3)
    relation = (1 - late) * (2 + 2 * side) + late * 6 + core
    return relation, (1 - late) * near + late * corner


def fused_kernel(
    density_ref, eig_ref, screen_ref, start_ref, len_ref, slot_ref, occ_ref, out_ref,
    density, extra, extra_out, extra_meta, meta, keep, eig, screen, part, sent, from_edge, from_mid,
    proj, acc, place, high, low, sig_out, sig_own, sig_in, xy_out, xy_in, band_sum, fin_in,
    load_sem, swap_send, swap_recv, eig_send, eig_recv, z_send, z_recv, sig_send, sig_recv, xy_send, xy_recv,
    fin_send, fin_recv,
):
    mesh_id = pl.DeviceIdType.MESH
    band, z = lax.axis_index("band"), lax.axis_index("pw")
    n_rel, depth, _ = eig.shape
    sizes = quarter_sizes(depth)
    span = proj.shape[1]
    padded = acc.shape[1] // 2
    half_rows = screen_ref.shape[0] // 2
    block = extra.shape[0]
    cols = density.shape[0]
    slots = cols // block
    most = cols - block
    n_z = fin_in.shape[0] + 1
    mate, across = z + 1 - 2 * lax.rem(z, 2), n_z - 1 - z
    inner = (z == 1) | (z == 2)
    edge = (z == 0) | (z == n_z - 1)
    whole_rows = pl.ds(0, depth)

    loads = [
        pltpu.make_async_copy(eig_ref, eig.at[0], load_sem.at[0]),
        pltpu.make_async_copy(density_ref.at[pl.ds(0, cols)], density, load_sem.at[1]),
    ] + [
        pltpu.make_async_copy(
            screen_ref.at[pl.ds(half * half_rows, half_rows)],
            screen.at[pl.ds(half * padded, half_rows), pl.ds(0, screen_ref.shape[1])],
            load_sem.at[2 + half],
        )
        for half in range(2)
    ]
    for load in loads[:2]:
        load.start()

    def fields(slot):
        live = slot_ref[slot] >= 0
        kept = jnp.where(live, len_ref[slot], 0).astype(jnp.float32)
        weight = jnp.where(live, 0.5 - occ_ref[jnp.maximum(slot_ref[slot], 0)], 0.5)
        first = start_ref[slot].astype(jnp.float32)
        row = lax.broadcasted_iota(jnp.int32, (8, block), 0)
        return jnp.where(row == 0, kept, jnp.where(row == 1, weight, first))

    extra_out[...] = fields(slots)
    for slot in range(slots):
        meta[slot] = fields(slot)

    barrier = pltpu.get_barrier_semaphore()
    for rel in range(1, n_rel):
        pl.semaphore_signal(barrier, inc=1, device_id=(flip(band, rel), z), device_id_type=mesh_id)
    for k in range(1, n_z):
        pl.semaphore_signal(
            barrier, inc=1, device_id=(band, lax.rem(z + k, n_z)), device_id_type=mesh_id
        )
    lanes = lax.broadcasted_iota(jnp.int32, (8, block), 1).astype(jnp.float32)
    for slot in range(slots):
        keep[:, slot * block : (slot + 1) * block] = jnp.where(lanes < meta[slot, 0:1], 1.0, 0.0)
    pl.semaphore_wait(barrier, n_rel - 1 + n_z - 1)

    def remote(source, target, send, recv, device):
        return pltpu.make_async_remote_copy(
            src_ref=source, dst_ref=target, send_sem=send, recv_sem=recv,
            device_id=device, device_id_type=mesh_id,
        )

    def first_row(quarter):
        if isinstance(quarter, int):
            return sum(sizes[:quarter])
        return pl.multiple_of(
            quarter * sizes[1] + lax.div(quarter + 3, 4) * (sizes[0] - sizes[1]), 16
        )

    def each(quarter, act):
        if isinstance(quarter, int):
            act(pl.ds(first_row(quarter), sizes[quarter]))
            return
        for first, stop in ((0, 1), (1, 3), (3, 4)):
            @pl.when((quarter >= first) & (quarter < stop))
            def _():
                act(pl.ds(first_row(quarter), sizes[first]))

    def lane_of(rel):
        return flip(band, rel) * depth

    def shifted(rel, rows):
        return pl.ds(pl.multiple_of(rows.start + lax.rem(lane_of(rel), 128), 16), rows.size)

    def own_copy(rel, quarter, rows):
        return remote(
            eig_ref.at[rows], eig.at[rel, rows], eig_send.at[rel, quarter],
            eig_recv.at[rel, quarter], (flip(band, rel), z),
        )

    def forward_copy(rel, quarter, rows):
        return remote(
            eig.at[rel, rows], eig.at[rel + 1, rows], eig_send.at[rel + 1, quarter],
            eig_recv.at[rel + 1, quarter], (flip(band, 1), z),
        )

    def corner_copy(via, quarter, rows):
        return remote(
            eig.at[via, rows], eig.at[6, rows], eig_send.at[6, quarter],
            eig_recv.at[6, quarter], (flip(band, 6 - via), z),
        )

    def landed(rel, quarter, rows):
        return remote(
            eig.at[rel, rows], eig.at[rel, rows], eig_send.at[rel, quarter],
            eig_recv.at[rel, quarter], (flip(band, 1), z),
        )

    def z_copy(kind, rel, quarter, rows, columns):
        source, target = ((sent, from_edge), (sent, from_mid), (proj, proj))[kind]
        if kind == 2:
            rows = shifted(rel, rows)
        return remote(
            source.at[rel, rows, columns], target.at[rel, rows, columns],
            z_send.at[kind, rel, quarter], z_recv.at[kind, rel, quarter],
            (band, across if kind == 1 else mate),
        )

    swaps = [
        remote(source, target, swap_send.at[index], swap_recv.at[index], (flip(band, 4), z))
        for index, (source, target) in enumerate(
            [(density_ref.at[pl.ds(cols, block)], extra), (extra_out, extra_meta)]
        )
    ]
    for swap in swaps:
        swap.start()
    for index in range(N_QUARTER):
        for rel, quarter in ((1, index), (2, index), (4, (index + 1) % N_QUARTER)):
            each(quarter, lambda rows: own_copy(rel, quarter, rows).start())

    first_cols, last_cols, all_cols = pl.ds(0, most), pl.ds(most, block), pl.ds(0, cols)

    proj[...] = jnp.zeros_like(proj)
    acc[...] = jnp.zeros_like(acc)
    for half in range(2):
        screen[half * padded + half_rows : (half + 1) * padded] = jnp.zeros(
            (padded - half_rows, screen.shape[1]), screen.dtype
        )
    screen[:, screen_ref.shape[1] :] = jnp.zeros(
        (screen.shape[0], screen.shape[1] - screen_ref.shape[1]), screen.dtype
    )

    def items(index, act):
        @pl.when((index >= 0) & (index < EARLY))
        def _():
            rel, quarter = lax.rem(index, 2), lax.div(index, 2)
            each(quarter, lambda rows: act(rel, quarter, rows, first_cols))

        @pl.when((index >= EARLY) & (index < EARLY + PATCH))
        def _():
            act(index - EARLY, N_QUARTER, whole_rows, last_cols)

        @pl.when((index >= EARLY + PATCH) & (index < TICKS))
        def _():
            rel, quarter = piece_of(index - EARLY - PATCH)
            each(quarter, lambda rows: act(rel, quarter, rows, all_cols))

    def arrive(index):
        @pl.when((index < EARLY) & (lax.rem(index, 2) == 1))
        def _():
            quarter = lax.div(index, 2)
            each(quarter, lambda rows: landed(1, quarter, rows).wait_recv())

        @pl.when(index == EARLY)
        def _():
            for swap in swaps:
                swap.wait_recv()
            taken = meta[slots - 1, 0:1, 0:1] > 0.0
            meta[slots - 1] = jnp.where(taken, meta[slots - 1], extra_meta[...])
            density[most:] = jnp.where(taken, density[most:], extra[...])
            keep[:, most:] = jnp.where(lanes < meta[slots - 1, 0:1], 1.0, 0.0)

        @pl.when((index >= EARLY + PATCH) & (index < TICKS))
        def _():
            rel, quarter = piece_of(index - EARLY - PATCH)
            each(quarter, lambda rows: landed(rel, quarter, rows).wait_recv())

            @pl.when(lax.rem(rel, 2) == 0)
            def _():
                each(quarter, lambda rows: forward_copy(rel, quarter, rows).start())

            @pl.when((rel == 2) & (quarter == 0))
            def _():
                each(0, lambda rows: corner_copy(2, 0, rows).start())

            @pl.when((rel == 4) & (quarter > 0))
            def _():
                each(quarter, lambda rows: corner_copy(4, quarter, rows).start())

    def project(rel, quarter, rows, columns):
        result = lax.dot_general(
            eig[rel, rows], density[columns], (((1,), (1,)), ((), ())),
            preferred_element_type=jnp.float32,
        )
        part[rel, rows, columns] = result
        sent[rel, rows, columns] = result.astype(jnp.bfloat16)

        @pl.when(edge)
        def _():
            z_copy(0, rel, quarter, rows, columns).start()

    def add_edge(rel, quarter, rows, columns):
        z_copy(0, rel, quarter, rows, columns).wait_recv()
        total = part[rel, rows, columns] + from_edge[rel, rows, columns].astype(jnp.float32)
        part[rel, rows, columns] = total
        sent[rel, rows, columns] = total.astype(jnp.bfloat16)
        z_copy(1, rel, quarter, rows, columns).start()

    def add_mid(rel, quarter, rows, columns):
        z_copy(1, rel, quarter, rows, columns).wait_recv()
        total = part[rel, rows, columns] + from_mid[rel, rows, columns].astype(jnp.float32)
        proj[rel, shifted(rel, rows), columns] = (total * keep[0:1, columns]).astype(jnp.bfloat16)
        z_copy(2, rel, quarter, rows, columns).start()

    def apply_screen(rel):
        @pl.when(edge)
        def _():
            for columns, some in ((first_cols, rel < 2), (all_cols, rel >= 2)):
                @pl.when(some)
                def _():
                    for quarter in range(N_QUARTER):
                        each(
                            quarter,
                            lambda rows: z_copy(2, rel, quarter, rows, columns).wait_recv(),
                        )

            @pl.when(rel < 2)
            def _():
                z_copy(2, rel, N_QUARTER, whole_rows, last_cols).wait_recv()

        lane = pl.multiple_of(lax.div(lane_of(rel), 128) * 128, 128)
        acc[...] += lax.dot_general(
            proj[rel], screen[:, pl.ds(lane, span)],
            (((0,), (1,)), ((), ())), preferred_element_type=jnp.float32,
        )

    strip = place.shape[1]

    def build_place():
        for slot in range(slots):
            here = slice(slot * block, (slot + 1) * block)
            window = lax.broadcasted_iota(jnp.int32, (strip, block), 1).astype(jnp.float32)
            window = window + meta[slot, 2:3]
            bands = lax.broadcasted_iota(jnp.int32, (strip, block), 0).astype(jnp.float32)
            for index in range(n_rel):
                same = bands + float(index * strip) == window
                place[index, :, here] = jnp.where(same, 1.0, 0.0).astype(jnp.bfloat16)

    def step(t, carry):
        arrive(t)
        items(t, project)

        @pl.when(inner)
        def _():
            items(t - LAG_SUM, add_edge)
            items(t - LAG_TOTAL, add_mid)

        @pl.when(t == EARLY + 4)
        def _():
            build_place()
            for load in loads[2:]:
                load.wait()

        done = t - LAG_SCREEN
        ready = done == DONE[0]
        for index in DONE[1:]:
            ready = ready | (done == index)

        @pl.when(ready)
        def _():
            late = lax.div(done, EARLY + PATCH)
            late = lax.div(late + 3, 4)
            apply_screen(
                (1 - late) * (done - EARLY) + late * piece_of(late * (done - EARLY - PATCH))[0]
            )

        return carry

    loads[0].wait()
    loads[1].wait()
    for load in loads[2:]:
        load.start()
    lax.fori_loop(0, TICKS + LAG_SCREEN, step, 0)

    pair = []
    for half in range(2):
        rel = flip(band, 2 * z + half)
        pair.append((rel, shifted(rel, pl.ds(0, padded))))
    for slot in range(slots):
        here = slice(slot * block, (slot + 1) * block)
        other = jnp.concatenate([proj[rel, rows, here] for rel, rows in pair], axis=0)
        total = jnp.dot(
            jnp.concatenate(split(acc[here]), axis=0), other, preferred_element_type=jnp.float32
        )
        total = (total[:block] + total[block:]) * meta[slot, 1:2]
        spread = lax.dot_general(
            jnp.concatenate(split(total), axis=0),
            place[:, :, here].reshape(n_rel * strip, block), (((1,), (1,)), ((), ())),
            preferred_element_type=jnp.float32,
        )
        high[here], low[here] = split(spread[:block] + spread[block:])

    core = lax.rem(band, 2)
    chip = lax.div(band, 2)

    def strips(parity):
        rows = jnp.concatenate([place[2 * index + parity] for index in range(n_rel // 2)], axis=0)
        return sum(
            jnp.dot(rows, value[...], preferred_element_type=jnp.float32) for value in (high, low)
        ).reshape(sig_out.shape)

    sig_out[...] = strips(1 - core)
    core_copy = remote(sig_out, sig_in, sig_send, sig_recv, (flip(band, 1), z))
    core_copy.start()
    sig_own[...] = strips(core)

    def chip_copy(rel):
        target = flip(band, 2 * rel)
        return remote(
            xy_out.at[lax.div(target, 2)], xy_in.at[rel - 1], xy_send.at[rel - 1],
            xy_recv.at[rel - 1], (target, z),
        )

    def final_copy(k):
        target = lax.rem(z + k, n_z)
        return remote(
            band_sum.at[target], fin_in.at[k - 1], fin_send.at[k - 1], fin_recv.at[k - 1],
            (band, target),
        )

    core_copy.wait_recv()
    sig_own[...] += sig_in[...]
    xy_out[...] = sig_own[...].astype(jnp.bfloat16)
    for rel in (3, 1, 2):
        chip_copy(rel).start()

    for swap in swaps:
        swap.wait_send()

    def drain_z(rel, quarter, rows, columns):
        @pl.when(edge)
        def _():
            z_copy(0, rel, quarter, rows, columns).wait_send()

        @pl.when(inner)
        def _():
            z_copy(1, rel, quarter, rows, columns).wait_send()
            z_copy(2, rel, quarter, rows, columns).wait_send()

    def drain(rel, carry):
        for quarter in range(N_QUARTER):
            @pl.when(rel > 0)
            def _():
                each(quarter, lambda rows: landed(rel, quarter, rows).wait_send())

            @pl.when(rel < 2)
            def _():
                each(quarter, lambda rows: drain_z(rel, quarter, rows, first_cols))

            @pl.when(rel >= 2)
            def _():
                each(quarter, lambda rows: drain_z(rel, quarter, rows, all_cols))

        @pl.when(rel < 2)
        def _():
            drain_z(rel, N_QUARTER, whole_rows, last_cols)

        return carry

    lax.fori_loop(0, n_rel, drain, 0)
    core_copy.wait_send()

    total = sig_own[chip]
    for rel in range(1, 4):
        chip_copy(rel).wait_recv()
        total = total + xy_in[rel - 1].astype(jnp.float32)
    band_sum[...] = total.reshape(band_sum.shape)
    for k in (2, 1, 3):
        final_copy(k).start()
    total = band_sum[z]
    for k in range(1, n_z):
        final_copy(k).wait_recv()
        total = total + fin_in[k - 1]
    out_ref[...] = total
    for rel in range(1, 4):
        chip_copy(rel).wait_send()
    for k in range(1, n_z):
        final_copy(k).wait_send()


def per_device(
    n_z, n_rel, pair_density, eigvecs, screening, occupation, window_start, window_len, slot_band
):
    capacity, block, plane_rows = pair_density.shape
    depth, width = eigvecs.shape[0], screening.shape[0]
    slots = capacity - 1
    cols = slots * block
    half_rows = -(-(width // 2) // 128) * 128
    span = -(-(depth + 112) // 128) * 128
    lanes = -(-screening.shape[1] // 128) * 128 + 128
    dma = pltpu.SemaphoreType.DMA
    vmem = pl.BlockSpec(memory_space=pltpu.VMEM)
    smem = pl.BlockSpec(memory_space=pltpu.SMEM)
    hbm = pl.BlockSpec(memory_space=pl.ANY)
    strip = NB_SIGMA // n_rel
    fine = strip // n_z
    f32, bf16 = jnp.float32, jnp.bfloat16
    return pl.pallas_call(
        fused_kernel,
        out_shape=jax.ShapeDtypeStruct((fine, NB_SIGMA), f32),
        in_specs=[hbm, hbm, hbm, smem, smem, smem, smem],
        out_specs=vmem,
        scratch_shapes=[
            pltpu.VMEM((cols, plane_rows), bf16),
            pltpu.VMEM((block, plane_rows), bf16),
            pltpu.VMEM((8, block), f32),
            pltpu.VMEM((8, block), f32),
            pltpu.VMEM((slots, 8, block), f32),
            pltpu.VMEM((8, cols), f32),
            pltpu.VMEM((n_rel, depth, plane_rows), bf16),
            pltpu.VMEM((2 * half_rows, lanes), bf16),
            pltpu.VMEM((n_rel, depth, cols), f32),
            pltpu.VMEM((n_rel, depth, cols), bf16),
            pltpu.VMEM((n_rel, depth, cols), bf16),
            pltpu.VMEM((n_rel, depth, cols), bf16),
            pltpu.VMEM((n_rel, span, cols), bf16),
            pltpu.VMEM((cols, 2 * half_rows), f32),
            pltpu.VMEM((n_rel, strip, cols), bf16),
            pltpu.VMEM((cols, NB_SIGMA), bf16),
            pltpu.VMEM((cols, NB_SIGMA), bf16),
            pltpu.VMEM((n_rel // 2, strip, NB_SIGMA), f32),
            pltpu.VMEM((n_rel // 2, strip, NB_SIGMA), f32),
            pltpu.VMEM((n_rel // 2, strip, NB_SIGMA), f32),
            pltpu.VMEM((n_rel // 2, strip, NB_SIGMA), bf16),
            pltpu.VMEM((n_rel // 2 - 1, strip, NB_SIGMA), bf16),
            pltpu.VMEM((n_z, fine, NB_SIGMA), f32),
            pltpu.VMEM((n_z - 1, fine, NB_SIGMA), f32),
            dma((4,)),
            dma((2,)),
            dma((2,)),
            dma((n_rel, N_QUARTER)),
            dma((n_rel, N_QUARTER)),
            dma((3, n_rel, N_QUARTER + 1)),
            dma((3, n_rel, N_QUARTER + 1)),
            dma,
            dma,
            dma((n_rel // 2 - 1,)),
            dma((n_rel // 2 - 1,)),
            dma((n_z - 1,)),
            dma((n_z - 1,)),
        ],
        compiler_params=pltpu.CompilerParams(
            collective_id=0, has_side_effects=True, vmem_limit_bytes=60 * 2**20
        ),
    )(
        pair_density.reshape(capacity * block, plane_rows),
        eigvecs,
        screening,
        window_start,
        window_len,
        slot_band,
        occupation,
    )


def solution(mesh):
    n_band, n_z = mesh.shape["band"], mesh.shape["pw"]
    body = ring_per_device
    if n_band == 8 and n_z == 4:
        body = functools.partial(per_device, n_z, n_band)
    return jax.shard_map(
        body,
        mesh=mesh,
        in_specs=(
            P("band", None, "pw"),
            P("band", "pw"),
            P("pw", None),
            P(),
            P("band"),
            P("band"),
            P("band"),
        ),
        out_specs=P(("band", "pw"), None),
        check_vma=False,
    )
```

```python
import functools

import jax
import jax.numpy as jnp
from jax import lax
from jax.experimental import pallas as pl
from jax.experimental.pallas import tpu as pltpu
from jax.sharding import PartitionSpec as P

NB_SIGMA = 512


def ring_per_device(pair_density, eigvecs, screening, occupation, window_start, window_len, slot_band):
    capacity, block, plane_rows = pair_density.shape
    density, starts, lengths, band_ids = (pair_density, window_start, window_len, slot_band)
    slots = density.shape[0]
    flat = density.reshape(slots * block, plane_rows)
    partial_proj = lax.dot_general(
        flat,
        lax.all_gather(eigvecs, "band", axis=0, tiled=True),
        (((1,), (1,)), ((), ())),
        preferred_element_type=jnp.float32,
    )
    row_ids = jnp.arange(block, dtype=jnp.int32)
    keep_rows = ((row_ids[None, :] < lengths[:, None]) & (band_ids[:, None] >= 0)).astype(
        jnp.float32
    )
    masked = partial_proj * keep_rows.reshape(slots * block, 1)
    projected = lax.psum(masked, "pw").astype(jnp.bfloat16)
    width = screening.shape[0]
    own_cols = lax.dynamic_slice_in_dim(projected, lax.axis_index("pw") * width, width, 1)
    screened = lax.dot_general(
        projected, screening, (((1,), (1,)), ((), ())), preferred_element_type=jnp.float32
    ).astype(jnp.bfloat16)
    block_sigma = lax.dot_general(
        screened.reshape(slots, block, width),
        own_cols.reshape(slots, block, width),
        (((2,), (2,)), ((0,), (0,))),
        preferred_element_type=jnp.float32,
    )
    band_list = jnp.arange(occupation.shape[0], dtype=jnp.int32)
    weights = 0.5 - jnp.sum(
        jnp.where(band_list[None, :] == band_ids[:, None], occupation[None, :], 0.0), axis=1
    )
    totals = jnp.zeros((NB_SIGMA + block, NB_SIGMA + block), jnp.float32)
    for index in range(slots):
        first = starts[index]
        previous = lax.dynamic_slice(totals, (first, first), (block, block))
        totals = lax.dynamic_update_slice(
            totals, previous + weights[index] * block_sigma[index], (first, first)
        )
    sigma_part = totals[:NB_SIGMA, :NB_SIGMA]
    by_band = lax.psum_scatter(sigma_part, "band", scatter_dimension=0, tiled=True)
    return lax.psum_scatter(by_band, "pw", scatter_dimension=0, tiled=True)


def flip(index, relation):
    total = 0
    for place in (4, 2, 1):
        bit = lax.rem(index // place, 2)
        other = lax.rem(relation // place, 2)
        total = total + place * (bit + other - 2 * bit * other)
    return total


def split(value):
    top = value.astype(jnp.bfloat16)
    return top, (value - top.astype(jnp.float32)).astype(jnp.bfloat16)


N_QUARTER = 4
EARLY, PATCH, FULL = 2 * N_QUARTER, 2, 6 * N_QUARTER
TICKS = EARLY + PATCH + FULL
LAG_SUM, LAG_TOTAL, LAG_SCREEN = 2, 4, 6
ORDER = (
    (2, 0), (2, 1), (4, 1), (2, 2), (4, 2), (2, 3), (4, 3), (6, 1), (4, 0), (6, 2), (6, 0), (6, 3),
)
DONE = tuple(EARLY + rel for rel in range(2)) + tuple(
    EARLY + PATCH + 2 * max(at for at, pair in enumerate(ORDER) if pair[0] == rel) + core
    for rel in (2, 4, 6) for core in range(2)
)


def look_up(values, index):
    result = values[0]
    for at in range(1, len(values)):
        change = values[at] - values[at - 1]
        if change:
            result = result + change * lax.div(index + (64 - at), 64)
    return result


def quarter_sizes(depth):
    units = depth // 16
    middle = -(-units // N_QUARTER)
    return 16 * (middle + 1), 16 * middle, 16 * middle, 16 * (units - 3 * middle - 1)


def piece_of(order):
    pair, core = lax.div(order, 2), lax.rem(order, 2)
    code = look_up([8 * rel + quarter for rel, quarter in ORDER], pair)
    return lax.div(code, 8) + core, lax.rem(code, 8)


def fused_kernel(
    density_ref, eig_ref, screen_ref, start_ref, len_ref, slot_ref, occ_ref, out_ref,
    density, extra, extra_out, extra_meta, meta, keep, eig, screen, part, sent, from_edge, from_mid,
    proj, acc, place, high, low, sig_out, sig_own, sig_in, fin_out, fin_in,
    load_sem, swap_send, swap_recv, eig_send, eig_recv, z_send, z_recv, sig_send, sig_recv,
    fin_send, fin_recv,
):
    mesh_id = pl.DeviceIdType.MESH
    band, z = lax.axis_index("band"), lax.axis_index("pw")
    n_rel, depth, _ = eig.shape
    sizes = quarter_sizes(depth)
    span = proj.shape[1]
    padded = acc.shape[1] // 2
    half_rows = screen_ref.shape[0] // 2
    block = extra.shape[0]
    cols = density.shape[0]
    slots = cols // block
    most = cols - block
    n_z = fin_out.shape[1]
    fine = fin_out.shape[2]
    mate, across = z + 1 - 2 * lax.rem(z, 2), n_z - 1 - z
    inner = (z == 1) | (z == 2)
    edge = (z == 0) | (z == n_z - 1)
    whole_rows = pl.ds(0, depth)

    loads = [
        pltpu.make_async_copy(eig_ref, eig.at[0], load_sem.at[0]),
        pltpu.make_async_copy(density_ref.at[pl.ds(0, cols)], density, load_sem.at[1]),
    ] + [
        pltpu.make_async_copy(
            screen_ref.at[pl.ds(half * half_rows, half_rows)],
            screen.at[pl.ds(half * padded, half_rows), pl.ds(0, screen_ref.shape[1])],
            load_sem.at[2 + half],
        )
        for half in range(2)
    ]
    for load in loads[:2]:
        load.start()

    def fields(slot):
        live = slot_ref[slot] >= 0
        kept = jnp.where(live, len_ref[slot], 0).astype(jnp.float32)
        weight = jnp.where(live, 0.5 - occ_ref[jnp.maximum(slot_ref[slot], 0)], 0.5)
        first = start_ref[slot].astype(jnp.float32)
        row = lax.broadcasted_iota(jnp.int32, (8, block), 0)
        return jnp.where(row == 0, kept, jnp.where(row == 1, weight, first))

    extra_out[...] = fields(slots)
    for slot in range(slots):
        meta[slot] = fields(slot)

    barrier = pltpu.get_barrier_semaphore()
    for rel in range(1, n_rel):
        pl.semaphore_signal(barrier, inc=1, device_id=(flip(band, rel), z), device_id_type=mesh_id)
    for k in range(1, n_z):
        pl.semaphore_signal(
            barrier, inc=1, device_id=(band, lax.rem(z + k, n_z)), device_id_type=mesh_id
        )
    lanes = lax.broadcasted_iota(jnp.int32, (8, block), 1).astype(jnp.float32)
    for slot in range(slots):
        keep[:, slot * block : (slot + 1) * block] = jnp.where(lanes < meta[slot, 0:1], 1.0, 0.0)
    proj[...] = jnp.zeros_like(proj)
    acc[...] = jnp.zeros_like(acc)
    for half in range(2):
        screen[half * padded + half_rows : (half + 1) * padded] = jnp.zeros(
            (padded - half_rows, screen.shape[1]), screen.dtype
        )
    screen[:, screen_ref.shape[1] :] = jnp.zeros(
        (screen.shape[0], screen.shape[1] - screen_ref.shape[1]), screen.dtype
    )
    pl.semaphore_wait(barrier, n_rel - 1 + n_z - 1)

    def remote(source, target, send, recv, device):
        return pltpu.make_async_remote_copy(
            src_ref=source, dst_ref=target, send_sem=send, recv_sem=recv,
            device_id=device, device_id_type=mesh_id,
        )

    def first_row(quarter):
        if isinstance(quarter, int):
            return sum(sizes[:quarter])
        return pl.multiple_of(
            quarter * sizes[1] + lax.div(quarter + 3, 4) * (sizes[0] - sizes[1]), 16
        )

    def each(quarter, act):
        if isinstance(quarter, int):
            act(pl.ds(first_row(quarter), sizes[quarter]))
            return
        for first, stop in ((0, 1), (1, 3), (3, 4)):
            @pl.when((quarter >= first) & (quarter < stop))
            def _():
                act(pl.ds(first_row(quarter), sizes[first]))

    def lane_of(rel):
        return flip(band, rel) * depth

    def shifted(rel, rows):
        return pl.ds(pl.multiple_of(rows.start + lax.rem(lane_of(rel), 128), 16), rows.size)

    def own_copy(rel, quarter, rows):
        return remote(
            eig_ref.at[rows], eig.at[rel, rows], eig_send.at[rel, quarter],
            eig_recv.at[rel, quarter], (flip(band, rel), z),
        )

    def forward_copy(rel, quarter, rows):
        return remote(
            eig.at[rel, rows], eig.at[rel + 1, rows], eig_send.at[rel + 1, quarter],
            eig_recv.at[rel + 1, quarter], (flip(band, 1), z),
        )

    def corner_copy(via, quarter, rows):
        return remote(
            eig.at[via, rows], eig.at[6, rows], eig_send.at[6, quarter],
            eig_recv.at[6, quarter], (flip(band, 6 - via), z),
        )

    def landed(rel, quarter, rows):
        return remote(
            eig.at[rel, rows], eig.at[rel, rows], eig_send.at[rel, quarter],
            eig_recv.at[rel, quarter], (flip(band, 1), z),
        )

    def z_copy(kind, rel, quarter, rows, columns):
        source, target = ((sent, from_edge), (sent, from_mid), (proj, proj))[kind]
        if kind == 2:
            rows = shifted(rel, rows)
        return remote(
            source.at[rel, rows, columns], target.at[rel, rows, columns],
            z_send.at[kind, rel, quarter], z_recv.at[kind, rel, quarter],
            (band, across if kind == 1 else mate),
        )

    swaps = [
        remote(source, target, swap_send.at[index], swap_recv.at[index], (flip(band, 4), z))
        for index, (source, target) in enumerate(
            [(density_ref.at[pl.ds(cols, block)], extra), (extra_out, extra_meta)]
        )
    ]
    for swap in swaps:
        swap.start()
    for index in range(N_QUARTER):
        for rel, quarter in ((1, index), (2, index), (4, (index + 1) % N_QUARTER)):
            each(quarter, lambda rows: own_copy(rel, quarter, rows).start())

    first_cols, last_cols, all_cols = pl.ds(0, most), pl.ds(most, block), pl.ds(0, cols)

    def items(index, act):
        @pl.when((index >= 0) & (index < EARLY))
        def _():
            rel, quarter = lax.rem(index, 2), lax.div(index, 2)
            each(quarter, lambda rows: act(rel, quarter, rows, first_cols))

        @pl.when((index >= EARLY) & (index < EARLY + PATCH))
        def _():
            act(index - EARLY, N_QUARTER, whole_rows, last_cols)

        @pl.when((index >= EARLY + PATCH) & (index < TICKS))
        def _():
            rel, quarter = piece_of(index - EARLY - PATCH)
            each(quarter, lambda rows: act(rel, quarter, rows, all_cols))

    def arrive(index):
        @pl.when((index < EARLY) & (lax.rem(index, 2) == 1))
        def _():
            quarter = lax.div(index, 2)
            each(quarter, lambda rows: landed(1, quarter, rows).wait_recv())

        @pl.when(index == EARLY)
        def _():
            for swap in swaps:
                swap.wait_recv()
            taken = meta[slots - 1, 0:1, 0:1] > 0.0
            meta[slots - 1] = jnp.where(taken, meta[slots - 1], extra_meta[...])
            density[most:] = jnp.where(taken, density[most:], extra[...])
            keep[:, most:] = jnp.where(lanes < meta[slots - 1, 0:1], 1.0, 0.0)

        @pl.when((index >= EARLY + PATCH) & (index < TICKS))
        def _():
            rel, quarter = piece_of(index - EARLY - PATCH)
            each(quarter, lambda rows: landed(rel, quarter, rows).wait_recv())

            @pl.when(lax.rem(rel, 2) == 0)
            def _():
                each(quarter, lambda rows: forward_copy(rel, quarter, rows).start())

            @pl.when((rel == 2) & (quarter == 0))
            def _():
                each(0, lambda rows: corner_copy(2, 0, rows).start())

            @pl.when((rel == 4) & (quarter > 0))
            def _():
                each(quarter, lambda rows: corner_copy(4, quarter, rows).start())

    def project(rel, quarter, rows, columns):
        result = lax.dot_general(
            eig[rel, rows], density[columns], (((1,), (1,)), ((), ())),
            preferred_element_type=jnp.float32,
        )
        part[rel, rows, columns] = result
        sent[rel, rows, columns] = result.astype(jnp.bfloat16)

        @pl.when(edge)
        def _():
            z_copy(0, rel, quarter, rows, columns).start()

    def add_edge(rel, quarter, rows, columns):
        z_copy(0, rel, quarter, rows, columns).wait_recv()
        total = part[rel, rows, columns] + from_edge[rel, rows, columns].astype(jnp.float32)
        part[rel, rows, columns] = total
        sent[rel, rows, columns] = total.astype(jnp.bfloat16)
        z_copy(1, rel, quarter, rows, columns).start()

    def add_mid(rel, quarter, rows, columns):
        z_copy(1, rel, quarter, rows, columns).wait_recv()
        total = part[rel, rows, columns] + from_mid[rel, rows, columns].astype(jnp.float32)
        proj[rel, shifted(rel, rows), columns] = (total * keep[0:1, columns]).astype(jnp.bfloat16)
        z_copy(2, rel, quarter, rows, columns).start()

    def apply_screen(rel):
        @pl.when(edge)
        def _():
            for columns, some in ((first_cols, rel < 2), (all_cols, rel >= 2)):
                @pl.when(some)
                def _():
                    for quarter in range(N_QUARTER):
                        each(
                            quarter,
                            lambda rows: z_copy(2, rel, quarter, rows, columns).wait_recv(),
                        )

            @pl.when(rel < 2)
            def _():
                z_copy(2, rel, N_QUARTER, whole_rows, last_cols).wait_recv()

        lane = pl.multiple_of(lax.div(lane_of(rel), 128) * 128, 128)
        acc[...] += lax.dot_general(
            proj[rel], screen[:, pl.ds(lane, span)],
            (((0,), (1,)), ((), ())), preferred_element_type=jnp.float32,
        )

    strip = place.shape[1]

    def build_place():
        for slot in range(slots):
            here = slice(slot * block, (slot + 1) * block)
            window = lax.broadcasted_iota(jnp.int32, (strip, block), 1).astype(jnp.float32)
            window = window + meta[slot, 2:3]
            bands = lax.broadcasted_iota(jnp.int32, (strip, block), 0).astype(jnp.float32)
            for index in range(n_rel):
                same = bands + float(index * strip) == window
                place[index, :, here] = jnp.where(same, 1.0, 0.0).astype(jnp.bfloat16)

    def step(t, carry):
        arrive(t)
        items(t, project)

        @pl.when(inner)
        def _():
            items(t - LAG_SUM, add_edge)
            items(t - LAG_TOTAL, add_mid)

        @pl.when(t == EARLY + 4)
        def _():
            build_place()
            for load in loads[2:]:
                load.wait()

        done = t - LAG_SCREEN
        ready = done == DONE[0]
        for index in DONE[1:]:
            ready = ready | (done == index)

        @pl.when(ready)
        def _():
            late = lax.div(done, EARLY + PATCH)
            late = lax.div(late + 3, 4)
            apply_screen(
                (1 - late) * (done - EARLY) + late * piece_of(late * (done - EARLY - PATCH))[0]
            )

        return carry

    loads[0].wait()
    loads[1].wait()
    for load in loads[2:]:
        load.start()
    lax.fori_loop(0, TICKS + LAG_SCREEN, step, 0)

    pair = []
    for half in range(2):
        rel = flip(band, 2 * z + half)
        pair.append((rel, shifted(rel, pl.ds(0, padded))))
    for slot in range(slots):
        here = slice(slot * block, (slot + 1) * block)
        other = jnp.concatenate([proj[rel, rows, here] for rel, rows in pair], axis=0)
        total = jnp.dot(
            jnp.concatenate(split(acc[here]), axis=0), other, preferred_element_type=jnp.float32
        )
        total = (total[:block] + total[block:]) * meta[slot, 1:2]
        spread = lax.dot_general(
            jnp.concatenate(split(total), axis=0),
            place[:, :, here].reshape(n_rel * strip, block), (((1,), (1,)), ((), ())),
            preferred_element_type=jnp.float32,
        )
        high[here], low[here] = split(spread[:block] + spread[block:])

    core = lax.rem(band, 2)
    chip = lax.div(band, 2)

    def strips(parity):
        rows = jnp.concatenate([place[2 * index + parity] for index in range(n_rel // 2)], axis=0)
        return sum(
            jnp.dot(rows, value[...], preferred_element_type=jnp.float32) for value in (high, low)
        ).reshape(sig_out.shape)

    sig_out[...] = strips(1 - core)
    core_copy = remote(sig_out, sig_in, sig_send, sig_recv, (flip(band, 1), z))
    core_copy.start()
    sig_own[...] = strips(core)

    def final_copy(rel, k):
        chip_to, z_to = flip(band, 2 * rel), lax.rem(z + k, n_z)
        at = rel * n_z + k - 1
        return remote(
            fin_out.at[lax.div(chip_to, 2), z_to], fin_in.at[at], fin_send.at[at], fin_recv.at[at],
            (chip_to, z_to),
        )

    finals = [
        final_copy(rel, k) for rel in (3, 1, 2, 0) for k in (2, 1, 3, 0) if rel + k > 0
    ]
    core_copy.wait_recv()
    sig_own[...] += sig_in[...]
    fin_out[...] = sig_own[...].astype(jnp.bfloat16).reshape(fin_out.shape)
    for copy in finals:
        copy.start()

    for swap in swaps:
        swap.wait_send()

    def drain_z(rel, quarter, rows, columns):
        @pl.when(edge)
        def _():
            z_copy(0, rel, quarter, rows, columns).wait_send()

        @pl.when(inner)
        def _():
            z_copy(1, rel, quarter, rows, columns).wait_send()
            z_copy(2, rel, quarter, rows, columns).wait_send()

    def drain(rel, carry):
        for quarter in range(N_QUARTER):
            @pl.when(rel > 0)
            def _():
                each(quarter, lambda rows: landed(rel, quarter, rows).wait_send())

            @pl.when(rel < 2)
            def _():
                each(quarter, lambda rows: drain_z(rel, quarter, rows, first_cols))

            @pl.when(rel >= 2)
            def _():
                each(quarter, lambda rows: drain_z(rel, quarter, rows, all_cols))

        @pl.when(rel < 2)
        def _():
            drain_z(rel, N_QUARTER, whole_rows, last_cols)

        return carry

    lax.fori_loop(0, n_rel, drain, 0)
    core_copy.wait_send()

    total = sig_own[chip, pl.ds(pl.multiple_of(z * fine, fine), fine)]
    for copy in finals:
        copy.wait_recv()
    for at in range(fin_in.shape[0]):
        total = total + fin_in[at].astype(jnp.float32)
    out_ref[...] = total
    for copy in finals:
        copy.wait_send()


def per_device(
    n_z, n_rel, pair_density, eigvecs, screening, occupation, window_start, window_len, slot_band
):
    capacity, block, plane_rows = pair_density.shape
    depth, width = eigvecs.shape[0], screening.shape[0]
    slots = capacity - 1
    cols = slots * block
    half_rows = -(-(width // 2) // 128) * 128
    span = -(-(depth + 112) // 128) * 128
    lanes = -(-screening.shape[1] // 128) * 128 + 128
    dma = pltpu.SemaphoreType.DMA
    vmem = pl.BlockSpec(memory_space=pltpu.VMEM)
    smem = pl.BlockSpec(memory_space=pltpu.SMEM)
    hbm = pl.BlockSpec(memory_space=pl.ANY)
    strip = NB_SIGMA // n_rel
    fine = strip // n_z
    f32, bf16 = jnp.float32, jnp.bfloat16
    return pl.pallas_call(
        fused_kernel,
        out_shape=jax.ShapeDtypeStruct((fine, NB_SIGMA), f32),
        in_specs=[hbm, hbm, hbm, smem, smem, smem, smem],
        out_specs=vmem,
        scratch_shapes=[
            pltpu.VMEM((cols, plane_rows), bf16),
            pltpu.VMEM((block, plane_rows), bf16),
            pltpu.VMEM((8, block), f32),
            pltpu.VMEM((8, block), f32),
            pltpu.VMEM((slots, 8, block), f32),
            pltpu.VMEM((8, cols), f32),
            pltpu.VMEM((n_rel, depth, plane_rows), bf16),
            pltpu.VMEM((2 * half_rows, lanes), bf16),
            pltpu.VMEM((n_rel, depth, cols), f32),
            pltpu.VMEM((n_rel, depth, cols), bf16),
            pltpu.VMEM((n_rel, depth, cols), bf16),
            pltpu.VMEM((n_rel, depth, cols), bf16),
            pltpu.VMEM((n_rel, span, cols), bf16),
            pltpu.VMEM((cols, 2 * half_rows), f32),
            pltpu.VMEM((n_rel, strip, cols), bf16),
            pltpu.VMEM((cols, NB_SIGMA), bf16),
            pltpu.VMEM((cols, NB_SIGMA), bf16),
            pltpu.VMEM((n_rel // 2, strip, NB_SIGMA), f32),
            pltpu.VMEM((n_rel // 2, strip, NB_SIGMA), f32),
            pltpu.VMEM((n_rel // 2, strip, NB_SIGMA), f32),
            pltpu.VMEM((n_rel // 2, n_z, fine, NB_SIGMA), bf16),
            pltpu.VMEM((n_rel // 2 * n_z - 1, fine, NB_SIGMA), bf16),
            dma((4,)),
            dma((2,)),
            dma((2,)),
            dma((n_rel, N_QUARTER)),
            dma((n_rel, N_QUARTER)),
            dma((3, n_rel, N_QUARTER + 1)),
            dma((3, n_rel, N_QUARTER + 1)),
            dma,
            dma,
            dma((n_rel // 2 * n_z - 1,)),
            dma((n_rel // 2 * n_z - 1,)),
        ],
        compiler_params=pltpu.CompilerParams(
            collective_id=0, has_side_effects=True, vmem_limit_bytes=60 * 2**20
        ),
    )(
        pair_density.reshape(capacity * block, plane_rows),
        eigvecs,
        screening,
        window_start,
        window_len,
        slot_band,
        occupation,
    )


def solution(mesh):
    n_band, n_z = mesh.shape["band"], mesh.shape["pw"]
    body = ring_per_device
    if n_band == 8 and n_z == 4:
        body = functools.partial(per_device, n_z, n_band)
    return jax.shard_map(
        body,
        mesh=mesh,
        in_specs=(
            P("band", None, "pw"),
            P("band", "pw"),
            P("pw", None),
            P(),
            P("band"),
            P("band"),
            P("band"),
        ),
        out_specs=P(("band", "pw"), None),
        check_vma=False,
    )
```

```python
import functools

import jax
import jax.numpy as jnp
from jax import lax
from jax.experimental import pallas as pl
from jax.experimental.pallas import tpu as pltpu
from jax.sharding import PartitionSpec as P

NB_SIGMA = 512


def ring_per_device(pair_density, eigvecs, screening, occupation, window_start, window_len, slot_band):
    capacity, block, plane_rows = pair_density.shape
    density, starts, lengths, band_ids = (pair_density, window_start, window_len, slot_band)
    slots = density.shape[0]
    flat = density.reshape(slots * block, plane_rows)
    partial_proj = lax.dot_general(
        flat,
        lax.all_gather(eigvecs, "band", axis=0, tiled=True),
        (((1,), (1,)), ((), ())),
        preferred_element_type=jnp.float32,
    )
    row_ids = jnp.arange(block, dtype=jnp.int32)
    keep_rows = ((row_ids[None, :] < lengths[:, None]) & (band_ids[:, None] >= 0)).astype(
        jnp.float32
    )
    masked = partial_proj * keep_rows.reshape(slots * block, 1)
    projected = lax.psum(masked, "pw").astype(jnp.bfloat16)
    width = screening.shape[0]
    own_cols = lax.dynamic_slice_in_dim(projected, lax.axis_index("pw") * width, width, 1)
    screened = lax.dot_general(
        projected, screening, (((1,), (1,)), ((), ())), preferred_element_type=jnp.float32
    ).astype(jnp.bfloat16)
    block_sigma = lax.dot_general(
        screened.reshape(slots, block, width),
        own_cols.reshape(slots, block, width),
        (((2,), (2,)), ((0,), (0,))),
        preferred_element_type=jnp.float32,
    )
    band_list = jnp.arange(occupation.shape[0], dtype=jnp.int32)
    weights = 0.5 - jnp.sum(
        jnp.where(band_list[None, :] == band_ids[:, None], occupation[None, :], 0.0), axis=1
    )
    totals = jnp.zeros((NB_SIGMA + block, NB_SIGMA + block), jnp.float32)
    for index in range(slots):
        first = starts[index]
        previous = lax.dynamic_slice(totals, (first, first), (block, block))
        totals = lax.dynamic_update_slice(
            totals, previous + weights[index] * block_sigma[index], (first, first)
        )
    sigma_part = totals[:NB_SIGMA, :NB_SIGMA]
    by_band = lax.psum_scatter(sigma_part, "band", scatter_dimension=0, tiled=True)
    return lax.psum_scatter(by_band, "pw", scatter_dimension=0, tiled=True)


def flip(index, relation):
    total = 0
    for place in (4, 2, 1):
        bit = lax.rem(index // place, 2)
        other = lax.rem(relation // place, 2)
        total = total + place * (bit + other - 2 * bit * other)
    return total


def split(value):
    top = value.astype(jnp.bfloat16)
    return top, (value - top.astype(jnp.float32)).astype(jnp.bfloat16)


N_QUARTER = 4
EARLY, PATCH, FULL = 2 * N_QUARTER, 2, 6 * N_QUARTER
TICKS = EARLY + PATCH + FULL
LAG_SUM, LAG_TOTAL, LAG_SCREEN = 2, 4, 6
ORDER = (
    (2, 0), (2, 1), (4, 1), (2, 2), (4, 2), (2, 3), (4, 3), (6, 1), (4, 0), (6, 2), (6, 0), (6, 3),
)
DONE = tuple(EARLY + rel for rel in range(2)) + tuple(
    EARLY + PATCH + 2 * max(at for at, pair in enumerate(ORDER) if pair[0] == rel) + core
    for rel in (2, 4, 6) for core in range(2)
)


def look_up(values, index):
    result = values[0]
    for at in range(1, len(values)):
        change = values[at] - values[at - 1]
        if change:
            result = result + change * lax.div(index + (64 - at), 64)
    return result


def quarter_sizes(depth):
    units = depth // 16
    middle = -(-units // N_QUARTER)
    return 16 * (middle + 1), 16 * middle, 16 * middle, 16 * (units - 3 * middle - 1)


def piece_of(order):
    pair, core = lax.div(order, 2), lax.rem(order, 2)
    code = look_up([8 * rel + quarter for rel, quarter in ORDER], pair)
    return lax.div(code, 8) + core, lax.rem(code, 8)


def fused_kernel(
    density_ref, eig_ref, screen_ref, start_hbm, len_hbm, slot_hbm, occ_hbm, out_ref,
    start_ref, len_ref, slot_ref, occ_ref,
    density, extra, extra_out, extra_meta, meta, keep, eig, screen, part, sent, from_edge, from_mid,
    proj, acc, place, high, low, sig_out, sig_own, sig_in, fin_out, fin_in,
    load_sem, swap_send, swap_recv, eig_send, eig_recv, z_send, z_recv, sig_send, sig_recv,
    fin_send, fin_recv,
):
    mesh_id = pl.DeviceIdType.MESH
    band, z = lax.axis_index("band"), lax.axis_index("pw")
    n_rel, depth, _ = eig.shape
    sizes = quarter_sizes(depth)
    span = proj.shape[1]
    padded = acc.shape[1] // 2
    half_rows = screen_ref.shape[0] // 2
    block = extra.shape[0]
    cols = density.shape[0]
    slots = cols // block
    most = cols - block
    n_z = fin_out.shape[1]
    fine = fin_out.shape[2]
    mate, across = z + 1 - 2 * lax.rem(z, 2), n_z - 1 - z
    inner = (z == 1) | (z == 2)
    edge = (z == 0) | (z == n_z - 1)
    whole_rows = pl.ds(0, depth)

    loads = [
        pltpu.make_async_copy(eig_ref, eig.at[0], load_sem.at[0]),
        pltpu.make_async_copy(density_ref.at[pl.ds(0, cols)], density, load_sem.at[1]),
    ] + [
        pltpu.make_async_copy(
            screen_ref.at[pl.ds(half * half_rows, half_rows)],
            screen.at[pl.ds(half * padded, half_rows), pl.ds(0, screen_ref.shape[1])],
            load_sem.at[2 + half],
        )
        for half in range(2)
    ]
    tables = [
        pltpu.make_async_copy(source, target, load_sem.at[4 + index])
        for index, (source, target) in enumerate(
            [(start_hbm, start_ref), (len_hbm, len_ref), (slot_hbm, slot_ref), (occ_hbm, occ_ref)]
        )
    ]
    for load in tables + loads[:2]:
        load.start()

    def fields(slot):
        live = slot_ref[slot] >= 0
        kept = jnp.where(live, len_ref[slot], 0).astype(jnp.float32)
        weight = jnp.where(live, 0.5 - occ_ref[jnp.maximum(slot_ref[slot], 0)], 0.5)
        first = start_ref[slot].astype(jnp.float32)
        row = lax.broadcasted_iota(jnp.int32, (8, block), 0)
        return jnp.where(row == 0, kept, jnp.where(row == 1, weight, first))

    barrier = pltpu.get_barrier_semaphore()
    for device in ((flip(band, 1), z), (flip(band, 2), z), (flip(band, 4), z), (band, mate)):
        pl.semaphore_signal(barrier, inc=1, device_id=device, device_id_type=mesh_id)

    @pl.when(inner)
    def _():
        pl.semaphore_signal(barrier, inc=1, device_id=(band, across), device_id_type=mesh_id)

    proj[...] = jnp.zeros_like(proj)
    acc[...] = jnp.zeros_like(acc)
    for half in range(2):
        screen[half * padded + half_rows : (half + 1) * padded] = jnp.zeros(
            (padded - half_rows, screen.shape[1]), screen.dtype
        )
    screen[:, screen_ref.shape[1] :] = jnp.zeros(
        (screen.shape[0], screen.shape[1] - screen_ref.shape[1]), screen.dtype
    )

    for load in tables:
        load.wait()
    extra_out[...] = fields(slots)
    for slot in range(slots):
        meta[slot] = fields(slot)
    lanes = lax.broadcasted_iota(jnp.int32, (8, block), 1).astype(jnp.float32)
    for slot in range(slots):
        keep[:, slot * block : (slot + 1) * block] = jnp.where(lanes < meta[slot, 0:1], 1.0, 0.0)
    @pl.when(edge)
    def _():
        pl.semaphore_wait(barrier, 4)

    @pl.when(inner)
    def _():
        pl.semaphore_wait(barrier, 5)


    def remote(source, target, send, recv, device):
        return pltpu.make_async_remote_copy(
            src_ref=source, dst_ref=target, send_sem=send, recv_sem=recv,
            device_id=device, device_id_type=mesh_id,
        )

    def first_row(quarter):
        if isinstance(quarter, int):
            return sum(sizes[:quarter])
        return pl.multiple_of(
            quarter * sizes[1] + lax.div(quarter + 3, 4) * (sizes[0] - sizes[1]), 16
        )

    def each(quarter, act):
        if isinstance(quarter, int):
            act(pl.ds(first_row(quarter), sizes[quarter]))
            return
        for first, stop in ((0, 1), (1, 3), (3, 4)):
            @pl.when((quarter >= first) & (quarter < stop))
            def _():
                act(pl.ds(first_row(quarter), sizes[first]))

    def lane_of(rel):
        return flip(band, rel) * depth

    def shifted(rel, rows):
        return pl.ds(pl.multiple_of(rows.start + lax.rem(lane_of(rel), 128), 16), rows.size)

    def own_copy(rel, quarter, rows):
        return remote(
            eig_ref.at[rows], eig.at[rel, rows], eig_send,
            eig_recv.at[rel, quarter], (flip(band, rel), z),
        )

    def forward_copy(rel, quarter, rows):
        return remote(
            eig.at[rel, rows], eig.at[rel + 1, rows], eig_send,
            eig_recv.at[rel + 1, quarter], (flip(band, 1), z),
        )

    def corner_copy(via, quarter, rows):
        return remote(
            eig.at[via, rows], eig.at[6, rows], eig_send,
            eig_recv.at[6, quarter], (flip(band, 6 - via), z),
        )

    def landed(rel, quarter, rows):
        return remote(
            eig.at[rel, rows], eig.at[rel, rows], eig_send,
            eig_recv.at[rel, quarter], (flip(band, 1), z),
        )

    def z_slot(kind, rel, quarter):
        if kind == 2:
            return rel
        if isinstance(quarter, int) and quarter == N_QUARTER:
            return n_rel * N_QUARTER + rel
        return rel * N_QUARTER + quarter

    def z_copy(kind, rel, quarter, rows, columns):
        source, target = ((sent, from_edge), (sent, from_mid), (proj, proj))[kind]
        if kind == 2:
            rows = shifted(rel, rows)
        return remote(
            source.at[rel, rows, columns], target.at[rel, rows, columns],
            z_send.at[kind // 2], z_recv.at[kind % 2, z_slot(kind, rel, quarter)],
            (band, across if kind == 1 else mate),
        )

    swaps = [
        remote(source, target, swap_send.at[index], swap_recv.at[index], (flip(band, 4), z))
        for index, (source, target) in enumerate(
            [(density_ref.at[pl.ds(cols, block)], extra), (extra_out, extra_meta)]
        )
    ]
    for swap in swaps:
        swap.start()
    for index in range(N_QUARTER):
        for rel, quarter in ((1, index), (2, index), (4, (index + 1) % N_QUARTER)):
            each(quarter, lambda rows: own_copy(rel, quarter, rows).start())

    first_cols, last_cols, all_cols = pl.ds(0, most), pl.ds(most, block), pl.ds(0, cols)

    def items(index, act):
        @pl.when((index >= 0) & (index < EARLY))
        def _():
            rel, quarter = lax.rem(index, 2), lax.div(index, 2)
            each(quarter, lambda rows: act(rel, quarter, rows, first_cols))

        @pl.when((index >= EARLY) & (index < EARLY + PATCH))
        def _():
            act(index - EARLY, N_QUARTER, whole_rows, last_cols)

        @pl.when((index >= EARLY + PATCH) & (index < TICKS))
        def _():
            rel, quarter = piece_of(index - EARLY - PATCH)
            each(quarter, lambda rows: act(rel, quarter, rows, all_cols))

    def arrive(index):
        @pl.when((index < EARLY) & (lax.rem(index, 2) == 1))
        def _():
            quarter = lax.div(index, 2)
            each(quarter, lambda rows: landed(1, quarter, rows).wait_recv())

        @pl.when(index == EARLY)
        def _():
            for swap in swaps:
                swap.wait_recv()
            taken = meta[slots - 1, 0:1, 0:1] > 0.0
            meta[slots - 1] = jnp.where(taken, meta[slots - 1], extra_meta[...])
            density[most:] = jnp.where(taken, density[most:], extra[...])
            keep[:, most:] = jnp.where(lanes < meta[slots - 1, 0:1], 1.0, 0.0)

        @pl.when((index >= EARLY + PATCH) & (index < TICKS))
        def _():
            rel, quarter = piece_of(index - EARLY - PATCH)
            each(quarter, lambda rows: landed(rel, quarter, rows).wait_recv())

            @pl.when(lax.rem(rel, 2) == 0)
            def _():
                each(quarter, lambda rows: forward_copy(rel, quarter, rows).start())

            @pl.when((rel == 2) & (quarter == 0))
            def _():
                each(0, lambda rows: corner_copy(2, 0, rows).start())

            @pl.when((rel == 4) & (quarter > 0))
            def _():
                each(quarter, lambda rows: corner_copy(4, quarter, rows).start())

    def project(rel, quarter, rows, columns):
        result = lax.dot_general(
            eig[rel, rows], density[columns], (((1,), (1,)), ((), ())),
            preferred_element_type=jnp.float32,
        )
        part[rel, rows, columns] = result
        sent[rel, rows, columns] = result.astype(jnp.bfloat16)

        @pl.when(edge)
        def _():
            z_copy(0, rel, quarter, rows, columns).start()

    def add_edge(rel, quarter, rows, columns):
        z_copy(0, rel, quarter, rows, columns).wait_recv()
        total = part[rel, rows, columns] + from_edge[rel, rows, columns].astype(jnp.float32)
        part[rel, rows, columns] = total
        sent[rel, rows, columns] = total.astype(jnp.bfloat16)
        z_copy(1, rel, quarter, rows, columns).start()

    def add_mid(rel, quarter, rows, columns):
        z_copy(1, rel, quarter, rows, columns).wait_recv()
        total = part[rel, rows, columns] + from_mid[rel, rows, columns].astype(jnp.float32)
        proj[rel, shifted(rel, rows), columns] = (total * keep[0:1, columns]).astype(jnp.bfloat16)
        z_copy(2, rel, quarter, rows, columns).start()

    def apply_screen(rel):
        @pl.when(edge)
        def _():
            z_copy(2, rel, 0, whole_rows, all_cols).wait_recv()

        lane = pl.multiple_of(lax.div(lane_of(rel), 128) * 128, 128)
        acc[...] += lax.dot_general(
            proj[rel], screen[:, pl.ds(lane, span)],
            (((0,), (1,)), ((), ())), preferred_element_type=jnp.float32,
        )

    strip = place.shape[1]

    def build_place():
        for slot in range(slots):
            here = slice(slot * block, (slot + 1) * block)
            window = lax.broadcasted_iota(jnp.int32, (strip, block), 1).astype(jnp.float32)
            window = window + meta[slot, 2:3]
            bands = lax.broadcasted_iota(jnp.int32, (strip, block), 0).astype(jnp.float32)
            for index in range(n_rel):
                same = bands + float(index * strip) == window
                place[index, :, here] = jnp.where(same, 1.0, 0.0).astype(jnp.bfloat16)

    def step(t, carry):
        arrive(t)
        items(t, project)

        @pl.when(inner)
        def _():
            items(t - LAG_SUM, add_edge)
            items(t - LAG_TOTAL, add_mid)

        @pl.when(t == EARLY + 4)
        def _():
            build_place()
            for load in loads[2:]:
                load.wait()

        done = t - LAG_SCREEN
        ready = done == DONE[0]
        for index in DONE[1:]:
            ready = ready | (done == index)

        @pl.when(ready)
        def _():
            late = lax.div(done, EARLY + PATCH)
            late = lax.div(late + 3, 4)
            apply_screen(
                (1 - late) * (done - EARLY) + late * piece_of(late * (done - EARLY - PATCH))[0]
            )

        return carry

    loads[0].wait()
    loads[1].wait()
    for load in loads[2:]:
        load.start()
    lax.fori_loop(0, TICKS + LAG_SCREEN, step, 0)

    pair = []
    for half in range(2):
        rel = flip(band, 2 * z + half)
        pair.append((rel, shifted(rel, pl.ds(0, padded))))
    for slot in range(slots):
        here = slice(slot * block, (slot + 1) * block)
        other = jnp.concatenate([proj[rel, rows, here] for rel, rows in pair], axis=0)
        total = jnp.dot(
            jnp.concatenate(split(acc[here]), axis=0), other, preferred_element_type=jnp.float32
        )
        total = (total[:block] + total[block:]) * meta[slot, 1:2]
        spread = lax.dot_general(
            jnp.concatenate(split(total), axis=0),
            place[:, :, here].reshape(n_rel * strip, block), (((1,), (1,)), ((), ())),
            preferred_element_type=jnp.float32,
        )
        high[here], low[here] = split(spread[:block] + spread[block:])

    core = lax.rem(band, 2)
    chip = lax.div(band, 2)

    def strips(parity):
        rows = jnp.concatenate([place[2 * index + parity] for index in range(n_rel // 2)], axis=0)
        return sum(
            jnp.dot(rows, value[...], preferred_element_type=jnp.float32) for value in (high, low)
        ).reshape(sig_out.shape)

    sig_out[...] = strips(1 - core)
    core_copy = remote(sig_out, sig_in, sig_send, sig_recv, (flip(band, 1), z))
    core_copy.start()
    sig_own[...] = strips(core)

    def final_copy(rel, k):
        chip_to, z_to = flip(band, 2 * rel), lax.rem(z + k, n_z)
        at = rel * n_z + k - 1
        return remote(
            fin_out.at[lax.div(chip_to, 2), z_to], fin_in.at[at], fin_send, fin_recv,
            (chip_to, z_to),
        )

    finals = [
        final_copy(rel, k) for rel in (3, 1, 2, 0) for k in (2, 1, 3, 0) if rel + k > 0
    ]
    core_copy.wait_recv()
    sig_own[...] += sig_in[...]
    fin_out[...] = sig_own[...].astype(jnp.bfloat16).reshape(fin_out.shape)
    for copy in finals:
        copy.start()

    for swap in swaps:
        swap.wait_send()

    remote(eig.at[pl.ds(1, n_rel - 1)], eig.at[pl.ds(1, n_rel - 1)], eig_send, eig_recv.at[0, 0], (flip(band, 1), z)).wait_send()
    remote(sent, sent, z_send.at[0], z_recv.at[0, 0], (band, mate)).wait_send()

    @pl.when(inner)
    def _():
        remote(sent, sent, z_send.at[1], z_recv.at[0, 0], (band, mate)).wait_send()

    core_copy.wait_send()

    total = sig_own[chip, pl.ds(pl.multiple_of(z * fine, fine), fine)]
    everything = remote(fin_in, fin_in, fin_send, fin_recv, (band, mate))
    everything.wait_recv()
    for at in range(fin_in.shape[0]):
        total = total + fin_in[at].astype(jnp.float32)
    out_ref[...] = total
    everything.wait_send()


def per_device(
    n_z, n_rel, pair_density, eigvecs, screening, occupation, window_start, window_len, slot_band
):
    capacity, block, plane_rows = pair_density.shape
    depth, width = eigvecs.shape[0], screening.shape[0]
    slots = capacity - 1
    cols = slots * block
    half_rows = -(-(width // 2) // 128) * 128
    span = -(-(depth + 112) // 128) * 128
    lanes = -(-screening.shape[1] // 128) * 128 + 128
    dma = pltpu.SemaphoreType.DMA
    vmem = pl.BlockSpec(memory_space=pltpu.VMEM)
    hbm = pl.BlockSpec(memory_space=pl.ANY)
    strip = NB_SIGMA // n_rel
    fine = strip // n_z
    f32, bf16 = jnp.float32, jnp.bfloat16
    return pl.pallas_call(
        fused_kernel,
        out_shape=jax.ShapeDtypeStruct((fine, NB_SIGMA), f32),
        in_specs=[hbm] * 7,
        out_specs=vmem,
        scratch_shapes=[
            pltpu.SMEM(window_start.shape, jnp.int32),
            pltpu.SMEM(window_len.shape, jnp.int32),
            pltpu.SMEM(slot_band.shape, jnp.int32),
            pltpu.SMEM(occupation.shape, f32),
            pltpu.VMEM((cols, plane_rows), bf16),
            pltpu.VMEM((block, plane_rows), bf16),
            pltpu.VMEM((8, block), f32),
            pltpu.VMEM((8, block), f32),
            pltpu.VMEM((slots, 8, block), f32),
            pltpu.VMEM((8, cols), f32),
            pltpu.VMEM((n_rel, depth, plane_rows), bf16),
            pltpu.VMEM((2 * half_rows, lanes), bf16),
            pltpu.VMEM((n_rel, depth, cols), f32),
            pltpu.VMEM((n_rel, depth, cols), bf16),
            pltpu.VMEM((n_rel, depth, cols), bf16),
            pltpu.VMEM((n_rel, depth, cols), bf16),
            pltpu.VMEM((n_rel, span, cols), bf16),
            pltpu.VMEM((cols, 2 * half_rows), f32),
            pltpu.VMEM((n_rel, strip, cols), bf16),
            pltpu.VMEM((cols, NB_SIGMA), bf16),
            pltpu.VMEM((cols, NB_SIGMA), bf16),
            pltpu.VMEM((n_rel // 2, strip, NB_SIGMA), f32),
            pltpu.VMEM((n_rel // 2, strip, NB_SIGMA), f32),
            pltpu.VMEM((n_rel // 2, strip, NB_SIGMA), f32),
            pltpu.VMEM((n_rel // 2, n_z, fine, NB_SIGMA), bf16),
            pltpu.VMEM((n_rel // 2 * n_z - 1, fine, NB_SIGMA), bf16),
            dma((8,)),
            dma((2,)),
            dma((2,)),
            dma,
            dma((n_rel, N_QUARTER)),
            dma((2,)),
            dma((2, n_rel * N_QUARTER + 2)),
            dma,
            dma,
            dma,
            dma,
        ],
        compiler_params=pltpu.CompilerParams(
            collective_id=0, has_side_effects=True, vmem_limit_bytes=60 * 2**20
        ),
    )(
        pair_density.reshape(capacity * block, plane_rows),
        eigvecs,
        screening,
        window_start,
        window_len,
        slot_band,
        occupation,
    )


def solution(mesh):
    n_band, n_z = mesh.shape["band"], mesh.shape["pw"]
    body = ring_per_device
    if n_band == 8 and n_z == 4:
        body = functools.partial(per_device, n_z, n_band)
    return jax.shard_map(
        body,
        mesh=mesh,
        in_specs=(
            P("band", None, "pw"),
            P("band", "pw"),
            P("pw", None),
            P(),
            P("band"),
            P("band"),
            P("band"),
        ),
        out_specs=P(("band", "pw"), None),
        check_vma=False,
    )
```

```python
import functools

import jax
import jax.numpy as jnp
from jax import lax
from jax.experimental import pallas as pl
from jax.experimental.pallas import tpu as pltpu
from jax.sharding import PartitionSpec as P

NB_SIGMA = 512


def ring_per_device(pair_density, eigvecs, screening, occupation, window_start, window_len, slot_band):
    capacity, block, plane_rows = pair_density.shape
    density, starts, lengths, band_ids = (pair_density, window_start, window_len, slot_band)
    slots = density.shape[0]
    flat = density.reshape(slots * block, plane_rows)
    partial_proj = lax.dot_general(
        flat,
        lax.all_gather(eigvecs, "band", axis=0, tiled=True),
        (((1,), (1,)), ((), ())),
        preferred_element_type=jnp.float32,
    )
    row_ids = jnp.arange(block, dtype=jnp.int32)
    keep_rows = ((row_ids[None, :] < lengths[:, None]) & (band_ids[:, None] >= 0)).astype(
        jnp.float32
    )
    masked = partial_proj * keep_rows.reshape(slots * block, 1)
    projected = lax.psum(masked, "pw").astype(jnp.bfloat16)
    width = screening.shape[0]
    own_cols = lax.dynamic_slice_in_dim(projected, lax.axis_index("pw") * width, width, 1)
    screened = lax.dot_general(
        projected, screening, (((1,), (1,)), ((), ())), preferred_element_type=jnp.float32
    ).astype(jnp.bfloat16)
    block_sigma = lax.dot_general(
        screened.reshape(slots, block, width),
        own_cols.reshape(slots, block, width),
        (((2,), (2,)), ((0,), (0,))),
        preferred_element_type=jnp.float32,
    )
    band_list = jnp.arange(occupation.shape[0], dtype=jnp.int32)
    weights = 0.5 - jnp.sum(
        jnp.where(band_list[None, :] == band_ids[:, None], occupation[None, :], 0.0), axis=1
    )
    totals = jnp.zeros((NB_SIGMA + block, NB_SIGMA + block), jnp.float32)
    for index in range(slots):
        first = starts[index]
        previous = lax.dynamic_slice(totals, (first, first), (block, block))
        totals = lax.dynamic_update_slice(
            totals, previous + weights[index] * block_sigma[index], (first, first)
        )
    sigma_part = totals[:NB_SIGMA, :NB_SIGMA]
    by_band = lax.psum_scatter(sigma_part, "band", scatter_dimension=0, tiled=True)
    return lax.psum_scatter(by_band, "pw", scatter_dimension=0, tiled=True)


def flip(index, relation):
    total = 0
    for place in (4, 2, 1):
        bit = lax.rem(index // place, 2)
        other = lax.rem(relation // place, 2)
        total = total + place * (bit + other - 2 * bit * other)
    return total


def split(value):
    top = value.astype(jnp.bfloat16)
    return top, (value - top.astype(jnp.float32)).astype(jnp.bfloat16)


N_PIECE = 5
EARLY, PATCH, FULL = 2 * N_PIECE, 2, 6 * N_PIECE
TICKS = EARLY + PATCH + FULL
LAG_SUM, LAG_TOTAL, LAG_SCREEN = 2, 4, 8
ORDER = (
    (2, 0), (2, 1), (2, 2), (4, 1), (4, 2), (2, 3), (4, 3), (2, 4), (4, 0), (6, 1), (4, 4), (6, 2),
    (6, 0), (6, 3), (6, 4),
)
Y_FIRST, X_FIRST = (1, 2, 3, 0, 4), (0, 1, 2, 3, 4)
DONE = tuple(EARLY + rel for rel in range(2)) + tuple(
    EARLY + PATCH + 2 * max(at for at, pair in enumerate(ORDER) if pair[0] == rel) + core
    for rel in (2, 4, 6) for core in range(2)
)


def look_up(values, index):
    result = values[0]
    for at in range(1, len(values)):
        change = values[at] - values[at - 1]
        if change:
            result = result + change * lax.div(index + (64 - at), 64)
    return result


def piece_sizes(depth):
    units = depth // 16
    middle = -(-units // N_PIECE)
    rest = units - 3 * middle
    return 16 * (rest - rest // 2), 16 * middle, 16 * middle, 16 * middle, 16 * (rest // 2)


def piece_of(order):
    pair, core = lax.div(order, 2), lax.rem(order, 2)
    code = look_up([8 * rel + quarter for rel, quarter in ORDER], pair)
    return lax.div(code, 8) + core, lax.rem(code, 8)


def fused_kernel(
    density_ref, eig_ref, screen_ref, start_hbm, len_hbm, slot_hbm, occ_hbm, out_ref,
    start_ref, len_ref, slot_ref, occ_ref,
    density, extra, extra_out, extra_meta, meta, keep, eig, screen, part, sent, from_edge, from_mid,
    proj, acc, place, high, low, sig_out, sig_own, sig_in, fin_out, fin_in,
    load_sem, swap_send, swap_recv, eig_send, eig_recv, z_send, z_recv, sig_send, sig_recv,
    fin_send, fin_recv,
):
    mesh_id = pl.DeviceIdType.MESH
    band, z = lax.axis_index("band"), lax.axis_index("pw")
    n_rel, depth, _ = eig.shape
    sizes = piece_sizes(depth)
    span = proj.shape[1]
    padded = acc.shape[1] // 2
    half_rows = screen_ref.shape[0] // 2
    block = extra.shape[0]
    cols = density.shape[0]
    slots = cols // block
    most = cols - block
    n_z = fin_out.shape[1]
    fine = fin_out.shape[2]
    mate, across = z + 1 - 2 * lax.rem(z, 2), n_z - 1 - z
    inner = (z == 1) | (z == 2)
    edge = (z == 0) | (z == n_z - 1)
    whole_rows = pl.ds(0, depth)

    loads = [
        pltpu.make_async_copy(eig_ref, eig.at[0], load_sem.at[0]),
        pltpu.make_async_copy(density_ref.at[pl.ds(0, cols)], density, load_sem.at[1]),
    ] + [
        pltpu.make_async_copy(
            screen_ref.at[pl.ds(half * half_rows, half_rows)],
            screen.at[pl.ds(half * padded, half_rows), pl.ds(0, screen_ref.shape[1])],
            load_sem.at[2 + half],
        )
        for half in range(2)
    ]
    tables = [
        pltpu.make_async_copy(source, target, load_sem.at[4 + index])
        for index, (source, target) in enumerate(
            [(start_hbm, start_ref), (len_hbm, len_ref), (slot_hbm, slot_ref), (occ_hbm, occ_ref)]
        )
    ]
    for load in tables + loads[:2]:
        load.start()

    def fields(slot):
        live = slot_ref[slot] >= 0
        kept = jnp.where(live, len_ref[slot], 0).astype(jnp.float32)
        weight = jnp.where(live, 0.5 - occ_ref[jnp.maximum(slot_ref[slot], 0)], 0.5)
        first = start_ref[slot].astype(jnp.float32)
        row = lax.broadcasted_iota(jnp.int32, (8, block), 0)
        return jnp.where(row == 0, kept, jnp.where(row == 1, weight, first))

    barrier = pltpu.get_barrier_semaphore()
    for device in ((flip(band, 1), z), (flip(band, 2), z), (flip(band, 4), z), (band, mate)):
        pl.semaphore_signal(barrier, inc=1, device_id=device, device_id_type=mesh_id)

    @pl.when(inner)
    def _():
        pl.semaphore_signal(barrier, inc=1, device_id=(band, across), device_id_type=mesh_id)

    proj[...] = jnp.zeros_like(proj)
    acc[...] = jnp.zeros_like(acc)
    for half in range(2):
        screen[half * padded + half_rows : (half + 1) * padded] = jnp.zeros(
            (padded - half_rows, screen.shape[1]), screen.dtype
        )
    screen[:, screen_ref.shape[1] :] = jnp.zeros(
        (screen.shape[0], screen.shape[1] - screen_ref.shape[1]), screen.dtype
    )

    for load in tables:
        load.wait()
    extra_out[...] = fields(slots)
    for slot in range(slots):
        meta[slot] = fields(slot)
    lanes = lax.broadcasted_iota(jnp.int32, (8, block), 1).astype(jnp.float32)
    for slot in range(slots):
        keep[:, slot * block : (slot + 1) * block] = jnp.where(lanes < meta[slot, 0:1], 1.0, 0.0)
    @pl.when(edge)
    def _():
        pl.semaphore_wait(barrier, 4)

    @pl.when(inner)
    def _():
        pl.semaphore_wait(barrier, 5)


    def remote(source, target, send, recv, device):
        return pltpu.make_async_remote_copy(
            src_ref=source, dst_ref=target, send_sem=send, recv_sem=recv,
            device_id=device, device_id_type=mesh_id,
        )

    def first_row(quarter):
        if isinstance(quarter, int):
            return sum(sizes[:quarter])
        return pl.multiple_of(
            quarter * sizes[1] + lax.div(quarter + 7, 8) * (sizes[0] - sizes[1]), 16
        )

    def each(quarter, act):
        if isinstance(quarter, int):
            act(pl.ds(first_row(quarter), sizes[quarter]))
            return
        for first, stop in ((0, 1), (1, 4), (4, 5)):
            @pl.when((quarter >= first) & (quarter < stop))
            def _():
                act(pl.ds(first_row(quarter), sizes[first]))

    def lane_of(rel):
        return flip(band, rel) * depth

    def shifted(rel, rows):
        return pl.ds(pl.multiple_of(rows.start + lax.rem(lane_of(rel), 128), 16), rows.size)

    def own_copy(rel, quarter, rows):
        return remote(
            eig_ref.at[rows], eig.at[rel, rows], eig_send,
            eig_recv.at[rel, quarter], (flip(band, rel), z),
        )

    def forward_copy(rel, quarter, rows):
        return remote(
            eig.at[rel, rows], eig.at[rel + 1, rows], eig_send,
            eig_recv.at[rel + 1, quarter], (flip(band, 1), z),
        )

    def corner_copy(via, quarter, rows):
        return remote(
            eig.at[via, rows], eig.at[6, rows], eig_send,
            eig_recv.at[6, quarter], (flip(band, 6 - via), z),
        )

    def landed(rel, quarter, rows):
        return remote(
            eig.at[rel, rows], eig.at[rel, rows], eig_send,
            eig_recv.at[rel, quarter], (flip(band, 1), z),
        )

    def z_slot(kind, rel, quarter):
        if kind == 2:
            return rel
        if isinstance(quarter, int) and quarter == N_PIECE:
            return n_rel * N_PIECE + rel
        return rel * N_PIECE + quarter

    def z_copy(kind, rel, quarter, rows, columns):
        source, target = ((sent, from_edge), (sent, from_mid), (proj, proj))[kind]
        if kind == 2:
            rows = shifted(rel, rows)
        return remote(
            source.at[rel, rows, columns], target.at[rel, rows, columns],
            z_send.at[kind // 2], z_recv.at[kind % 2, z_slot(kind, rel, quarter)],
            (band, across if kind == 1 else mate),
        )

    swaps = [
        remote(source, target, swap_send.at[index], swap_recv.at[index], (flip(band, 4), z))
        for index, (source, target) in enumerate(
            [(density_ref.at[pl.ds(cols, block)], extra), (extra_out, extra_meta)]
        )
    ]
    for swap in swaps:
        swap.start()
    for index in range(N_PIECE):
        for rel, quarter in ((1, index), (2, X_FIRST[index]), (4, Y_FIRST[index])):
            each(quarter, lambda rows: own_copy(rel, quarter, rows).start())

    first_cols, last_cols, all_cols = pl.ds(0, most), pl.ds(most, block), pl.ds(0, cols)

    def items(index, act):
        @pl.when((index >= 0) & (index < EARLY))
        def _():
            rel, quarter = lax.rem(index, 2), lax.div(index, 2)
            each(quarter, lambda rows: act(rel, quarter, rows, first_cols))

        @pl.when((index >= EARLY) & (index < EARLY + PATCH))
        def _():
            act(index - EARLY, N_PIECE, whole_rows, last_cols)

        @pl.when((index >= EARLY + PATCH) & (index < TICKS))
        def _():
            rel, quarter = piece_of(index - EARLY - PATCH)
            each(quarter, lambda rows: act(rel, quarter, rows, all_cols))

    def arrive(index):
        @pl.when((index < EARLY) & (lax.rem(index, 2) == 1))
        def _():
            quarter = lax.div(index, 2)
            each(quarter, lambda rows: landed(1, quarter, rows).wait_recv())

        @pl.when(index == EARLY)
        def _():
            for swap in swaps:
                swap.wait_recv()
            taken = meta[slots - 1, 0:1, 0:1] > 0.0
            meta[slots - 1] = jnp.where(taken, meta[slots - 1], extra_meta[...])
            density[most:] = jnp.where(taken, density[most:], extra[...])
            keep[:, most:] = jnp.where(lanes < meta[slots - 1, 0:1], 1.0, 0.0)

        @pl.when((index >= EARLY + PATCH) & (index < TICKS))
        def _():
            rel, quarter = piece_of(index - EARLY - PATCH)
            each(quarter, lambda rows: landed(rel, quarter, rows).wait_recv())

            @pl.when(lax.rem(rel, 2) == 0)
            def _():
                each(quarter, lambda rows: forward_copy(rel, quarter, rows).start())

            outer = (quarter == 0) | (quarter == N_PIECE - 1)

            @pl.when((rel == 2) & outer)
            def _():
                each(quarter, lambda rows: corner_copy(2, quarter, rows).start())

            @pl.when((rel == 4) & (quarter > 0) & (quarter < N_PIECE - 1))
            def _():
                each(quarter, lambda rows: corner_copy(4, quarter, rows).start())

    def project(rel, quarter, rows, columns):
        result = lax.dot_general(
            eig[rel, rows], density[columns], (((1,), (1,)), ((), ())),
            preferred_element_type=jnp.float32,
        )
        part[rel, rows, columns] = result
        sent[rel, rows, columns] = result.astype(jnp.bfloat16)

        @pl.when(edge)
        def _():
            z_copy(0, rel, quarter, rows, columns).start()

    def add_edge(rel, quarter, rows, columns):
        z_copy(0, rel, quarter, rows, columns).wait_recv()
        total = part[rel, rows, columns] + from_edge[rel, rows, columns].astype(jnp.float32)
        part[rel, rows, columns] = total
        sent[rel, rows, columns] = total.astype(jnp.bfloat16)
        z_copy(1, rel, quarter, rows, columns).start()

    def add_mid(rel, quarter, rows, columns):
        z_copy(1, rel, quarter, rows, columns).wait_recv()
        total = part[rel, rows, columns] + from_mid[rel, rows, columns].astype(jnp.float32)
        proj[rel, shifted(rel, rows), columns] = (total * keep[0:1, columns]).astype(jnp.bfloat16)
        z_copy(2, rel, quarter, rows, columns).start()

    def apply_screen(rel):
        @pl.when(edge)
        def _():
            z_copy(2, rel, 0, whole_rows, all_cols).wait_recv()

        lane = pl.multiple_of(lax.div(lane_of(rel), 128) * 128, 128)
        acc[...] += lax.dot_general(
            proj[rel], screen[:, pl.ds(lane, span)],
            (((0,), (1,)), ((), ())), preferred_element_type=jnp.float32,
        )

    strip = place.shape[1]

    def build_place():
        for slot in range(slots):
            here = slice(slot * block, (slot + 1) * block)
            window = lax.broadcasted_iota(jnp.int32, (strip, block), 1).astype(jnp.float32)
            window = window + meta[slot, 2:3]
            bands = lax.broadcasted_iota(jnp.int32, (strip, block), 0).astype(jnp.float32)
            for index in range(n_rel):
                same = bands + float(index * strip) == window
                place[index, :, here] = jnp.where(same, 1.0, 0.0).astype(jnp.bfloat16)

    def step(t, carry):
        arrive(t)
        items(t, project)

        @pl.when(inner)
        def _():
            items(t - LAG_SUM, add_edge)
            items(t - LAG_TOTAL, add_mid)

        @pl.when(t == EARLY + 4)
        def _():
            build_place()
            for load in loads[2:]:
                load.wait()

        done = t - LAG_SCREEN
        ready = done == DONE[0]
        for index in DONE[1:]:
            ready = ready | (done == index)

        @pl.when(ready)
        def _():
            late = lax.div(done, EARLY + PATCH)
            late = lax.div(late + 3, 4)
            apply_screen(
                (1 - late) * (done - EARLY) + late * piece_of(late * (done - EARLY - PATCH))[0]
            )

        return carry

    loads[0].wait()
    loads[1].wait()
    for load in loads[2:]:
        load.start()
    lax.fori_loop(0, TICKS + LAG_SCREEN, step, 0)

    pair = []
    for half in range(2):
        rel = flip(band, 2 * z + half)
        pair.append((rel, shifted(rel, pl.ds(0, padded))))
    for slot in range(slots):
        here = slice(slot * block, (slot + 1) * block)
        other = jnp.concatenate([proj[rel, rows, here] for rel, rows in pair], axis=0)
        total = jnp.dot(
            jnp.concatenate(split(acc[here]), axis=0), other, preferred_element_type=jnp.float32
        )
        total = (total[:block] + total[block:]) * meta[slot, 1:2]
        spread = lax.dot_general(
            jnp.concatenate(split(total), axis=0),
            place[:, :, here].reshape(n_rel * strip, block), (((1,), (1,)), ((), ())),
            preferred_element_type=jnp.float32,
        )
        high[here], low[here] = split(spread[:block] + spread[block:])

    core = lax.rem(band, 2)
    chip = lax.div(band, 2)

    def strips(parity):
        rows = jnp.concatenate([place[2 * index + parity] for index in range(n_rel // 2)], axis=0)
        return sum(
            jnp.dot(rows, value[...], preferred_element_type=jnp.float32) for value in (high, low)
        ).reshape(sig_out.shape)

    sig_out[...] = strips(1 - core)
    core_copy = remote(sig_out, sig_in, sig_send, sig_recv, (flip(band, 1), z))
    core_copy.start()
    sig_own[...] = strips(core)

    def final_copy(rel, k):
        chip_to, z_to = flip(band, 2 * rel), lax.rem(z + k, n_z)
        at = rel * n_z + k - 1
        return remote(
            fin_out.at[lax.div(chip_to, 2), z_to], fin_in.at[at], fin_send, fin_recv,
            (chip_to, z_to),
        )

    finals = [
        final_copy(rel, k) for rel in (3, 1, 2, 0) for k in (2, 1, 3, 0) if rel + k > 0
    ]
    core_copy.wait_recv()
    sig_own[...] += sig_in[...]
    fin_out[...] = sig_own[...].astype(jnp.bfloat16).reshape(fin_out.shape)
    for copy in finals:
        copy.start()

    for swap in swaps:
        swap.wait_send()

    remote(eig.at[pl.ds(1, n_rel - 1)], eig.at[pl.ds(1, n_rel - 1)], eig_send, eig_recv.at[0, 0], (flip(band, 1), z)).wait_send()
    remote(sent, sent, z_send.at[0], z_recv.at[0, 0], (band, mate)).wait_send()

    @pl.when(inner)
    def _():
        remote(sent, sent, z_send.at[1], z_recv.at[0, 0], (band, mate)).wait_send()

    core_copy.wait_send()

    total = sig_own[chip, pl.ds(pl.multiple_of(z * fine, fine), fine)]
    everything = remote(fin_in, fin_in, fin_send, fin_recv, (band, mate))
    everything.wait_recv()
    for at in range(fin_in.shape[0]):
        total = total + fin_in[at].astype(jnp.float32)
    out_ref[...] = total
    everything.wait_send()


def per_device(
    n_z, n_rel, pair_density, eigvecs, screening, occupation, window_start, window_len, slot_band
):
    capacity, block, plane_rows = pair_density.shape
    depth, width = eigvecs.shape[0], screening.shape[0]
    slots = capacity - 1
    cols = slots * block
    half_rows = -(-(width // 2) // 128) * 128
    span = -(-(depth + 112) // 128) * 128
    lanes = -(-screening.shape[1] // 128) * 128 + 128
    dma = pltpu.SemaphoreType.DMA
    vmem = pl.BlockSpec(memory_space=pltpu.VMEM)
    hbm = pl.BlockSpec(memory_space=pl.ANY)
    strip = NB_SIGMA // n_rel
    fine = strip // n_z
    f32, bf16 = jnp.float32, jnp.bfloat16
    return pl.pallas_call(
        fused_kernel,
        out_shape=jax.ShapeDtypeStruct((fine, NB_SIGMA), f32),
        in_specs=[hbm] * 7,
        out_specs=vmem,
        scratch_shapes=[
            pltpu.SMEM(window_start.shape, jnp.int32),
            pltpu.SMEM(window_len.shape, jnp.int32),
            pltpu.SMEM(slot_band.shape, jnp.int32),
            pltpu.SMEM(occupation.shape, f32),
            pltpu.VMEM((cols, plane_rows), bf16),
            pltpu.VMEM((block, plane_rows), bf16),
            pltpu.VMEM((8, block), f32),
            pltpu.VMEM((8, block), f32),
            pltpu.VMEM((slots, 8, block), f32),
            pltpu.VMEM((8, cols), f32),
            pltpu.VMEM((n_rel, depth, plane_rows), bf16),
            pltpu.VMEM((2 * half_rows, lanes), bf16),
            pltpu.VMEM((n_rel, depth, cols), f32),
            pltpu.VMEM((n_rel, depth, cols), bf16),
            pltpu.VMEM((n_rel, depth, cols), bf16),
            pltpu.VMEM((n_rel, depth, cols), bf16),
            pltpu.VMEM((n_rel, span, cols), bf16),
            pltpu.VMEM((cols, 2 * half_rows), f32),
            pltpu.VMEM((n_rel, strip, cols), bf16),
            pltpu.VMEM((cols, NB_SIGMA), bf16),
            pltpu.VMEM((cols, NB_SIGMA), bf16),
            pltpu.VMEM((n_rel // 2, strip, NB_SIGMA), f32),
            pltpu.VMEM((n_rel // 2, strip, NB_SIGMA), f32),
            pltpu.VMEM((n_rel // 2, strip, NB_SIGMA), f32),
            pltpu.VMEM((n_rel // 2, n_z, fine, NB_SIGMA), bf16),
            pltpu.VMEM((n_rel // 2 * n_z - 1, fine, NB_SIGMA), bf16),
            dma((8,)),
            dma((2,)),
            dma((2,)),
            dma,
            dma((n_rel, N_PIECE)),
            dma((2,)),
            dma((2, n_rel * N_PIECE + 2)),
            dma,
            dma,
            dma,
            dma,
        ],
        compiler_params=pltpu.CompilerParams(
            collective_id=0, has_side_effects=True, vmem_limit_bytes=60 * 2**20
        ),
    )(
        pair_density.reshape(capacity * block, plane_rows),
        eigvecs,
        screening,
        window_start,
        window_len,
        slot_band,
        occupation,
    )


def solution(mesh):
    n_band, n_z = mesh.shape["band"], mesh.shape["pw"]
    body = ring_per_device
    if n_band == 8 and n_z == 4:
        body = functools.partial(per_device, n_z, n_band)
    return jax.shard_map(
        body,
        mesh=mesh,
        in_specs=(
            P("band", None, "pw"),
            P("band", "pw"),
            P("pw", None),
            P(),
            P("band"),
            P("band"),
            P("band"),
        ),
        out_specs=P(("band", "pw"), None),
        check_vma=False,
    )
```

```python
import functools

import jax
import jax.numpy as jnp
from jax import lax
from jax.experimental import pallas as pl
from jax.experimental.pallas import tpu as pltpu
from jax.sharding import PartitionSpec as P

NB_SIGMA = 512


def ring_per_device(pair_density, eigvecs, screening, occupation, window_start, window_len, slot_band):
    capacity, block, plane_rows = pair_density.shape
    density, starts, lengths, band_ids = (pair_density, window_start, window_len, slot_band)
    slots = density.shape[0]
    flat = density.reshape(slots * block, plane_rows)
    partial_proj = lax.dot_general(
        flat,
        lax.all_gather(eigvecs, "band", axis=0, tiled=True),
        (((1,), (1,)), ((), ())),
        preferred_element_type=jnp.float32,
    )
    row_ids = jnp.arange(block, dtype=jnp.int32)
    keep_rows = ((row_ids[None, :] < lengths[:, None]) & (band_ids[:, None] >= 0)).astype(
        jnp.float32
    )
    masked = partial_proj * keep_rows.reshape(slots * block, 1)
    projected = lax.psum(masked, "pw").astype(jnp.bfloat16)
    width = screening.shape[0]
    own_cols = lax.dynamic_slice_in_dim(projected, lax.axis_index("pw") * width, width, 1)
    screened = lax.dot_general(
        projected, screening, (((1,), (1,)), ((), ())), preferred_element_type=jnp.float32
    ).astype(jnp.bfloat16)
    block_sigma = lax.dot_general(
        screened.reshape(slots, block, width),
        own_cols.reshape(slots, block, width),
        (((2,), (2,)), ((0,), (0,))),
        preferred_element_type=jnp.float32,
    )
    band_list = jnp.arange(occupation.shape[0], dtype=jnp.int32)
    weights = 0.5 - jnp.sum(
        jnp.where(band_list[None, :] == band_ids[:, None], occupation[None, :], 0.0), axis=1
    )
    totals = jnp.zeros((NB_SIGMA + block, NB_SIGMA + block), jnp.float32)
    for index in range(slots):
        first = starts[index]
        previous = lax.dynamic_slice(totals, (first, first), (block, block))
        totals = lax.dynamic_update_slice(
            totals, previous + weights[index] * block_sigma[index], (first, first)
        )
    sigma_part = totals[:NB_SIGMA, :NB_SIGMA]
    by_band = lax.psum_scatter(sigma_part, "band", scatter_dimension=0, tiled=True)
    return lax.psum_scatter(by_band, "pw", scatter_dimension=0, tiled=True)


def flip(index, relation):
    total = 0
    for place in (4, 2, 1):
        bit = lax.rem(index // place, 2)
        other = lax.rem(relation // place, 2)
        total = total + place * (bit + other - 2 * bit * other)
    return total


def split(value):
    top = value.astype(jnp.bfloat16)
    return top, (value - top.astype(jnp.float32)).astype(jnp.bfloat16)


N_PIECE = 5
EARLY, PATCH, FULL = 2 * N_PIECE, 2, 6 * N_PIECE
TICKS = EARLY + PATCH + FULL
LAG_SUM, LAG_TOTAL, LAG_SCREEN = 2, 4, 8
ORDER = (
    (2, 0), (2, 1), (2, 2), (4, 1), (4, 2), (2, 3), (4, 3), (2, 4), (4, 0), (6, 1), (4, 4), (6, 2),
    (6, 0), (6, 3), (6, 4),
)
Y_FIRST, X_FIRST = (1, 2, 3, 0, 4), (0, 1, 2, 3, 4)
DONE = tuple(EARLY + rel for rel in range(2)) + tuple(
    EARLY + PATCH + 2 * max(at for at, pair in enumerate(ORDER) if pair[0] == rel) + core
    for rel in (2, 4, 6) for core in range(2)
)


def look_up(values, index):
    result = values[0]
    for at in range(1, len(values)):
        change = values[at] - values[at - 1]
        if change:
            result = result + change * lax.div(index + (64 - at), 64)
    return result


def piece_sizes(depth):
    units = depth // 16
    middle = -(-units // N_PIECE)
    rest = units - 3 * middle
    return 16 * (rest - rest // 2), 16 * middle, 16 * middle, 16 * middle, 16 * (rest // 2)


def piece_of(order):
    pair, core = lax.div(order, 2), lax.rem(order, 2)
    code = look_up([8 * rel + quarter for rel, quarter in ORDER], pair)
    return lax.div(code, 8) + core, lax.rem(code, 8)


def fused_kernel(
    density_ref, eig_ref, screen_ref, start_hbm, len_hbm, slot_hbm, occ_hbm, out_ref,
    start_ref, len_ref, slot_ref, occ_ref,
    density, extra, extra_out, extra_meta, meta, keep, eig, screen, part, sent, from_edge, from_mid,
    proj, acc, place, high, low, sig_out, sig_own, sig_in, fin_out, fin_in,
    load_sem, swap_send, swap_recv, eig_send, eig_recv, z_send, z_recv, sig_send, sig_recv,
    fin_send, fin_recv,
):
    mesh_id = pl.DeviceIdType.MESH
    band, z = lax.axis_index("band"), lax.axis_index("pw")
    n_rel, depth, _ = eig.shape
    sizes = piece_sizes(depth)
    span = proj.shape[1]
    padded = acc.shape[1] // 2
    half_rows = screen_ref.shape[0] // 2
    block = extra.shape[0]
    cols = density.shape[0]
    slots = cols // block
    most = cols - block
    n_z = fin_out.shape[1]
    fine = fin_out.shape[2]
    mate, across = z + 1 - 2 * lax.rem(z, 2), n_z - 1 - z
    inner = (z == 1) | (z == 2)
    edge = (z == 0) | (z == n_z - 1)
    whole_rows = pl.ds(0, depth)

    loads = [
        pltpu.make_async_copy(eig_ref, eig.at[0], load_sem.at[0]),
        pltpu.make_async_copy(density_ref.at[pl.ds(0, cols)], density, load_sem.at[1]),
    ] + [
        pltpu.make_async_copy(
            screen_ref.at[pl.ds(half * half_rows, half_rows)],
            screen.at[pl.ds(half * padded, half_rows), pl.ds(0, screen_ref.shape[1])],
            load_sem.at[2 + half],
        )
        for half in range(2)
    ]
    tables = [
        pltpu.make_async_copy(source, target, load_sem.at[4 + index])
        for index, (source, target) in enumerate(
            [(start_hbm, start_ref), (len_hbm, len_ref), (slot_hbm, slot_ref), (occ_hbm, occ_ref)]
        )
    ]
    for load in tables + loads[:2]:
        load.start()

    def fields(slot):
        live = slot_ref[slot] >= 0
        kept = jnp.where(live, len_ref[slot], 0).astype(jnp.float32)
        weight = jnp.where(live, 0.5 - occ_ref[jnp.maximum(slot_ref[slot], 0)], 0.5)
        first = start_ref[slot].astype(jnp.float32)
        row = lax.broadcasted_iota(jnp.int32, (8, block), 0)
        return jnp.where(row == 0, kept, jnp.where(row == 1, weight, first))

    barrier = pltpu.get_barrier_semaphore()
    for device in ((flip(band, 1), z), (flip(band, 2), z), (flip(band, 4), z), (band, mate)):
        pl.semaphore_signal(barrier, inc=1, device_id=device, device_id_type=mesh_id)

    @pl.when(inner)
    def _():
        pl.semaphore_signal(barrier, inc=1, device_id=(band, across), device_id_type=mesh_id)

    proj[...] = jnp.zeros_like(proj)
    acc[...] = jnp.zeros_like(acc)
    for half in range(2):
        screen[half * padded + half_rows : (half + 1) * padded] = jnp.zeros(
            (padded - half_rows, screen.shape[1]), screen.dtype
        )
    screen[:, screen_ref.shape[1] :] = jnp.zeros(
        (screen.shape[0], screen.shape[1] - screen_ref.shape[1]), screen.dtype
    )

    for load in tables:
        load.wait()
    extra_out[...] = fields(slots)
    for slot in range(slots):
        meta[slot] = fields(slot)
    lanes = lax.broadcasted_iota(jnp.int32, (8, block), 1).astype(jnp.float32)
    for slot in range(slots):
        keep[:, slot * block : (slot + 1) * block] = jnp.where(lanes < meta[slot, 0:1], 1.0, 0.0)
    @pl.when(edge)
    def _():
        pl.semaphore_wait(barrier, 4)

    @pl.when(inner)
    def _():
        pl.semaphore_wait(barrier, 5)


    def remote(source, target, send, recv, device):
        return pltpu.make_async_remote_copy(
            src_ref=source, dst_ref=target, send_sem=send, recv_sem=recv,
            device_id=device, device_id_type=mesh_id,
        )

    def first_row(quarter):
        if isinstance(quarter, int):
            return sum(sizes[:quarter])
        return pl.multiple_of(
            quarter * sizes[1] + lax.div(quarter + 7, 8) * (sizes[0] - sizes[1]), 16
        )

    def each(quarter, act):
        if isinstance(quarter, int):
            act(pl.ds(first_row(quarter), sizes[quarter]))
            return
        for first, stop in ((0, 1), (1, 4), (4, 5)):
            @pl.when((quarter >= first) & (quarter < stop))
            def _():
                act(pl.ds(first_row(quarter), sizes[first]))

    def lane_of(rel):
        return flip(band, rel) * depth

    def shifted(rel, rows):
        return pl.ds(pl.multiple_of(rows.start + lax.rem(lane_of(rel), 128), 16), rows.size)

    def own_copy(rel, quarter, rows):
        return remote(
            eig_ref.at[rows], eig.at[rel, rows], eig_send,
            eig_recv.at[rel, quarter], (flip(band, rel), z),
        )

    def forward_copy(rel, quarter, rows):
        return remote(
            eig.at[rel, rows], eig.at[rel + 1, rows], eig_send,
            eig_recv.at[rel + 1, quarter], (flip(band, 1), z),
        )

    def corner_copy(via, quarter, rows):
        return remote(
            eig.at[via, rows], eig.at[6, rows], eig_send,
            eig_recv.at[6, quarter], (flip(band, 6 - via), z),
        )

    def landed(rel, quarter, rows):
        return remote(
            eig.at[rel, rows], eig.at[rel, rows], eig_send,
            eig_recv.at[rel, quarter], (flip(band, 1), z),
        )

    def z_slot(kind, rel, quarter):
        if kind == 2:
            return rel
        if isinstance(quarter, int) and quarter == N_PIECE:
            return n_rel * N_PIECE + rel
        return rel * N_PIECE + quarter

    def z_copy(kind, rel, quarter, rows, columns):
        source, target = ((sent, from_edge), (sent, from_mid), (proj, proj))[kind]
        if kind == 2:
            rows = shifted(rel, rows)
        return remote(
            source.at[rel, rows, columns], target.at[rel, rows, columns],
            z_send.at[kind // 2], z_recv.at[kind % 2, z_slot(kind, rel, quarter)],
            (band, across if kind == 1 else mate),
        )

    swaps = [
        remote(source, target, swap_send.at[index], swap_recv.at[index], (flip(band, 4), z))
        for index, (source, target) in enumerate(
            [(density_ref.at[pl.ds(cols, block)], extra), (extra_out, extra_meta)]
        )
    ]
    for swap in swaps:
        swap.start()
    for index in range(N_PIECE):
        for rel, quarter in ((1, index), (2, X_FIRST[index]), (4, Y_FIRST[index])):
            each(quarter, lambda rows: own_copy(rel, quarter, rows).start())

    first_cols, last_cols, all_cols = pl.ds(0, most), pl.ds(most, block), pl.ds(0, cols)

    def items(index, act):
        @pl.when((index >= 0) & (index < EARLY))
        def _():
            rel, quarter = lax.rem(index, 2), lax.div(index, 2)
            each(quarter, lambda rows: act(rel, quarter, rows, first_cols))

        @pl.when((index >= EARLY) & (index < EARLY + PATCH))
        def _():
            act(index - EARLY, N_PIECE, whole_rows, last_cols)

        @pl.when((index >= EARLY + PATCH) & (index < TICKS))
        def _():
            rel, quarter = piece_of(index - EARLY - PATCH)
            each(quarter, lambda rows: act(rel, quarter, rows, all_cols))

    def arrive(index):
        @pl.when((index < EARLY) & (lax.rem(index, 2) == 1))
        def _():
            quarter = lax.div(index, 2)
            each(quarter, lambda rows: landed(1, quarter, rows).wait_recv())

        @pl.when(index == EARLY)
        def _():
            for swap in swaps:
                swap.wait_recv()
            taken = meta[slots - 1, 0:1, 0:1] > 0.0
            meta[slots - 1] = jnp.where(taken, meta[slots - 1], extra_meta[...])
            density[most:] = jnp.where(taken, density[most:], extra[...])
            keep[:, most:] = jnp.where(lanes < meta[slots - 1, 0:1], 1.0, 0.0)

        @pl.when((index >= EARLY + PATCH) & (index < TICKS))
        def _():
            rel, quarter = piece_of(index - EARLY - PATCH)
            each(quarter, lambda rows: landed(rel, quarter, rows).wait_recv())

            @pl.when(lax.rem(rel, 2) == 0)
            def _():
                each(quarter, lambda rows: forward_copy(rel, quarter, rows).start())

            outer = (quarter == 0) | (quarter == N_PIECE - 1)

            @pl.when((rel == 2) & outer)
            def _():
                each(quarter, lambda rows: corner_copy(2, quarter, rows).start())

            @pl.when((rel == 4) & (quarter > 0) & (quarter < N_PIECE - 1))
            def _():
                each(quarter, lambda rows: corner_copy(4, quarter, rows).start())

    def project(rel, quarter, rows, columns):
        result = lax.dot_general(
            eig[rel, rows], density[columns], (((1,), (1,)), ((), ())),
            preferred_element_type=jnp.float32,
        )
        part[rel, rows, columns] = result
        sent[rel, rows, columns] = result.astype(jnp.bfloat16)

        @pl.when(edge)
        def _():
            z_copy(0, rel, quarter, rows, columns).start()

    def add_edge(rel, quarter, rows, columns):
        z_copy(0, rel, quarter, rows, columns).wait_recv()
        total = part[rel, rows, columns] + from_edge[rel, rows, columns].astype(jnp.float32)
        part[rel, rows, columns] = total
        sent[rel, rows, columns] = total.astype(jnp.bfloat16)
        z_copy(1, rel, quarter, rows, columns).start()

    def add_mid(rel, quarter, rows, columns):
        z_copy(1, rel, quarter, rows, columns).wait_recv()
        total = part[rel, rows, columns] + from_mid[rel, rows, columns].astype(jnp.float32)
        proj[rel, shifted(rel, rows), columns] = (total * keep[0:1, columns]).astype(jnp.bfloat16)
        z_copy(2, rel, quarter, rows, columns).start()

    def apply_screen(rel):
        @pl.when(edge)
        def _():
            z_copy(2, rel, 0, whole_rows, all_cols).wait_recv()

        lane = pl.multiple_of(lax.div(lane_of(rel), 128) * 128, 128)
        acc[...] += lax.dot_general(
            proj[rel], screen[:, pl.ds(lane, span)],
            (((0,), (1,)), ((), ())), preferred_element_type=jnp.float32,
        )

    strip = place.shape[1]

    def build_place():
        for slot in range(slots):
            here = slice(slot * block, (slot + 1) * block)
            window = lax.broadcasted_iota(jnp.int32, (strip, block), 1).astype(jnp.float32)
            window = window + meta[slot, 2:3]
            bands = lax.broadcasted_iota(jnp.int32, (strip, block), 0).astype(jnp.float32)
            for index in range(n_rel):
                same = bands + float(index * strip) == window
                place[index, :, here] = jnp.where(same, 1.0, 0.0).astype(jnp.bfloat16)

    def step(t, carry):
        arrive(t)
        items(t, project)

        @pl.when(inner)
        def _():
            items(t - LAG_SUM, add_edge)
            items(t - LAG_TOTAL, add_mid)

        @pl.when(t == EARLY + 4)
        def _():
            build_place()
            for load in loads[2:]:
                load.wait()

        done = t - LAG_SCREEN
        ready = done == DONE[0]
        for index in DONE[1:]:
            ready = ready | (done == index)

        @pl.when(ready)
        def _():
            late = lax.div(done, EARLY + PATCH)
            late = lax.div(late + 3, 4)
            apply_screen(
                (1 - late) * (done - EARLY) + late * piece_of(late * (done - EARLY - PATCH))[0]
            )

        return carry

    loads[0].wait()
    loads[1].wait()
    for load in loads[2:]:
        load.start()
    lax.fori_loop(0, TICKS + LAG_SCREEN, step, 0)

    pair = []
    for half in range(2):
        rel = flip(band, 2 * z + half)
        pair.append((rel, shifted(rel, pl.ds(0, padded))))
    for slot in range(slots):
        here = slice(slot * block, (slot + 1) * block)
        other = jnp.concatenate([proj[rel, rows, here] for rel, rows in pair], axis=0)
        total = jnp.dot(
            jnp.concatenate(split(acc[here]), axis=0), other, preferred_element_type=jnp.float32
        )
        total = (total[:block] + total[block:]) * meta[slot, 1:2]
        spread = lax.dot_general(
            jnp.concatenate(split(total), axis=0),
            place[:, :, here].reshape(n_rel * strip, block), (((1,), (1,)), ((), ())),
            preferred_element_type=jnp.float32,
        )
        high[here], low[here] = split(spread[:block] + spread[block:])

    core = lax.rem(band, 2)
    chip = lax.div(band, 2)

    def strips(parity):
        rows = jnp.concatenate([place[2 * index + parity] for index in range(n_rel // 2)], axis=0)
        return sum(
            jnp.dot(rows, value[...], preferred_element_type=jnp.float32) for value in (high, low)
        ).reshape(sig_out.shape)

    sig_out[...] = strips(1 - core)
    core_copy = remote(sig_out, sig_in, sig_send, sig_recv, (flip(band, 1), z))
    core_copy.start()
    sig_own[...] = strips(core)

    def final_copy(rel, k):
        chip_to, z_to = flip(band, 2 * rel), lax.rem(z + k, n_z)
        at = rel * n_z + k - 1
        return remote(
            fin_out.at[lax.div(chip_to, 2), z_to], fin_in.at[at], fin_send, fin_recv,
            (chip_to, z_to),
        )

    finals = [
        final_copy(rel, k) for rel in (3, 2, 1, 0) for k in (2, 1, 3, 0) if rel + k > 0
    ]
    core_copy.wait_recv()
    sig_own[...] += sig_in[...]
    fin_out[...] = sig_own[...].astype(jnp.bfloat16).reshape(fin_out.shape)
    for copy in finals:
        copy.start()

    for swap in swaps:
        swap.wait_send()

    remote(eig.at[pl.ds(1, n_rel - 1)], eig.at[pl.ds(1, n_rel - 1)], eig_send, eig_recv.at[0, 0], (flip(band, 1), z)).wait_send()
    remote(sent, sent, z_send.at[0], z_recv.at[0, 0], (band, mate)).wait_send()

    @pl.when(inner)
    def _():
        remote(sent, sent, z_send.at[1], z_recv.at[0, 0], (band, mate)).wait_send()

    core_copy.wait_send()

    total = sig_own[chip, pl.ds(pl.multiple_of(z * fine, fine), fine)]
    everything = remote(fin_in, fin_in, fin_send, fin_recv, (band, mate))
    everything.wait_recv()
    for at in range(fin_in.shape[0]):
        total = total + fin_in[at].astype(jnp.float32)
    out_ref[...] = total
    everything.wait_send()


def per_device(
    n_z, n_rel, pair_density, eigvecs, screening, occupation, window_start, window_len, slot_band
):
    capacity, block, plane_rows = pair_density.shape
    depth, width = eigvecs.shape[0], screening.shape[0]
    slots = capacity - 1
    cols = slots * block
    half_rows = -(-(width // 2) // 128) * 128
    span = -(-(depth + 112) // 128) * 128
    lanes = -(-screening.shape[1] // 128) * 128 + 128
    dma = pltpu.SemaphoreType.DMA
    vmem = pl.BlockSpec(memory_space=pltpu.VMEM)
    hbm = pl.BlockSpec(memory_space=pl.ANY)
    strip = NB_SIGMA // n_rel
    fine = strip // n_z
    f32, bf16 = jnp.float32, jnp.bfloat16
    return pl.pallas_call(
        fused_kernel,
        out_shape=jax.ShapeDtypeStruct((fine, NB_SIGMA), f32),
        in_specs=[hbm] * 7,
        out_specs=vmem,
        scratch_shapes=[
            pltpu.SMEM(window_start.shape, jnp.int32),
            pltpu.SMEM(window_len.shape, jnp.int32),
            pltpu.SMEM(slot_band.shape, jnp.int32),
            pltpu.SMEM(occupation.shape, f32),
            pltpu.VMEM((cols, plane_rows), bf16),
            pltpu.VMEM((block, plane_rows), bf16),
            pltpu.VMEM((8, block), f32),
            pltpu.VMEM((8, block), f32),
            pltpu.VMEM((slots, 8, block), f32),
            pltpu.VMEM((8, cols), f32),
            pltpu.VMEM((n_rel, depth, plane_rows), bf16),
            pltpu.VMEM((2 * half_rows, lanes), bf16),
            pltpu.VMEM((n_rel, depth, cols), f32),
            pltpu.VMEM((n_rel, depth, cols), bf16),
            pltpu.VMEM((n_rel, depth, cols), bf16),
            pltpu.VMEM((n_rel, depth, cols), bf16),
            pltpu.VMEM((n_rel, span, cols), bf16),
            pltpu.VMEM((cols, 2 * half_rows), f32),
            pltpu.VMEM((n_rel, strip, cols), bf16),
            pltpu.VMEM((cols, NB_SIGMA), bf16),
            pltpu.VMEM((cols, NB_SIGMA), bf16),
            pltpu.VMEM((n_rel // 2, strip, NB_SIGMA), f32),
            pltpu.VMEM((n_rel // 2, strip, NB_SIGMA), f32),
            pltpu.VMEM((n_rel // 2, strip, NB_SIGMA), f32),
            pltpu.VMEM((n_rel // 2, n_z, fine, NB_SIGMA), bf16),
            pltpu.VMEM((n_rel // 2 * n_z - 1, fine, NB_SIGMA), bf16),
            dma((8,)),
            dma((2,)),
            dma((2,)),
            dma,
            dma((n_rel, N_PIECE)),
            dma((2,)),
            dma((2, n_rel * N_PIECE + 2)),
            dma,
            dma,
            dma,
            dma,
        ],
        compiler_params=pltpu.CompilerParams(
            collective_id=0, has_side_effects=True, vmem_limit_bytes=60 * 2**20
        ),
    )(
        pair_density.reshape(capacity * block, plane_rows),
        eigvecs,
        screening,
        window_start,
        window_len,
        slot_band,
        occupation,
    )


def solution(mesh):
    n_band, n_z = mesh.shape["band"], mesh.shape["pw"]
    body = ring_per_device
    if n_band == 8 and n_z == 4:
        body = functools.partial(per_device, n_z, n_band)
    return jax.shard_map(
        body,
        mesh=mesh,
        in_specs=(
            P("band", None, "pw"),
            P("band", "pw"),
            P("pw", None),
            P(),
            P("band"),
            P("band"),
            P("band"),
        ),
        out_specs=P(("band", "pw"), None),
        check_vma=False,
    )
```
